256 devices in a mesh: orb: 16 (over z, x_hi), cell: 16 (over y, x_lo, core).
Axes of the slice: x: 4 (x_hi: 2, x_lo: 2; x = x_hi * 2 + x_lo), y: 4, z: 8, core: 2. Of those that a mesh axis runs over, the one named last changes fastest.
Arguments:
- potentials: bfloat16 [192, 65536], P(None, 'cell'), may hold values from -6 to 6
- orbitals: bfloat16 [512, 65536], P('orb', 'cell'), may hold values from -6 to 6
- levels: float32 [512], replicated, may hold values from 0.2 to 4
- occ_index: int32 [128], replicated, may hold values from 0 to 511, as said below
- coul_rows: float32 [256, 256], replicated, may hold values from -0.375 to 0.375
- coul_cols: float32 [256, 256], replicated, may hold values from -0.375 to 0.375
Outputs:
- screened: float32 [192, 256, 256], P('orb', 'cell')
The draws below stay inside these ranges and needn't reach their ends.
Inputs may be any that keep to these rules, and one draw needn't show every extreme that they name: `occ_index`: 128 distinct orbital numbers.
All inputs are finite; a program needn't handle non-finite values.
Results may differ from the reference program's by a relative error of at most 0.004.
Values may be sent and summed in bfloat16 or wider, within the bound.
No kernel may reach another device: no remote copies, remote signals or barrier semaphores. Data moves between devices by JAX's collectives and lax.ppermute only.
A program may use at most 64 MiB of HBM per device.

```python
import math
import jax
import jax.numpy as jnp
from jax import lax

SIDE = 256
NORB = 512
NOCC = 128
NV = 192
POINTS = 65536


def draw_occ_index(key, part):
    return jax.random.permutation(jax.random.fold_in(key, 7), NORB)[:NOCC].astype(jnp.int32)


def block_levels(rng, extent, shards, low, largest):
    factor_of = 1.0
    for position, blocks in shards:
        heights = jax.random.uniform(jax.random.fold_in(jax.random.fold_in(rng, 6), position), (blocks,), jnp.float32, low / len(shards), largest / len(shards))
        factor_of = factor_of * jnp.repeat(jnp.exp(heights), extent[position] // blocks).reshape((-1,) + (1,) * (len(extent) - 1 - position))
    return factor_of


def centred(stream_key, shape, spread, bound, shards=(), kind=jnp.bfloat16):
    array = jax.random.normal(stream_key, shape, jnp.float32) * spread
    if len(shards) > 0:
        array = block_levels(stream_key, shape, shards, -0.22, 0.18) * array
    return jnp.clip(array, min=-bound, max=bound).astype(kind)


def setup_inputs(seed: int = 0) -> dict:
    arg_keys = jax.random.split(jax.random.key(seed), 7)
    potentials = centred(arg_keys[0], (NV, POINTS), 1.0, 6.0, ((1, 16),))
    orbitals = centred(arg_keys[1], (NORB, POINTS), 1.0, 6.0, ((0, 16), (1, 16)))
    levels = jnp.clip(jnp.exp(jax.random.uniform(arg_keys[2], (NORB,), jnp.float32, math.log(0.2), math.log(4.0))), 0.2, 4.0)
    occ_index = draw_occ_index(jax.random.fold_in(arg_keys[6], 71), 0)
    coul_rows = centred(arg_keys[4], (SIDE, SIDE), SIDE ** -0.5, 0.375, (), jnp.float32)
    coul_cols = centred(arg_keys[5], (SIDE, SIDE), SIDE ** -0.5, 0.375, (), jnp.float32)
    return dict(potentials=potentials, orbitals=orbitals, levels=levels, occ_index=occ_index, coul_rows=coul_rows, coul_cols=coul_cols)


def reference(potentials, orbitals, levels, occ_index, coul_rows, coul_cols):
    labels = jnp.arange(NORB, dtype=jnp.int32)
    marked = jnp.any(occ_index[:, None] == labels[None, :], axis=0)
    empty_mask = 1.0 - marked.astype(jnp.float32)
    volume = SIDE * SIDE
    basis = orbitals.astype(jnp.float32)

    def step(running, orbital_id):
        occ_row = lax.dynamic_index_in_dim(basis, orbital_id, 0, keepdims=False)
        products = (occ_row[None, :] * basis).astype(jnp.bfloat16)
        intersection = lax.dot_general(products, potentials, (((1,), (1,)), ((), ())), preferred_element_type=jnp.float32)
        occ_level = lax.dynamic_index_in_dim(levels, orbital_id, 0, keepdims=False)
        weights = -2.0 * empty_mask / (occ_level + levels)
        guess_block = (intersection * (weights / volume)[:, None]).astype(jnp.bfloat16)
        running = running + lax.dot_general(guess_block, products, (((0,), (0,)), ((), ())), preferred_element_type=jnp.float32)
        return running, None

    response, _ = lax.scan(step, jnp.zeros((NV, volume), jnp.float32), occ_index)
    plane = response.reshape(NV, SIDE, SIDE)
    by_columns = jnp.einsum("vrc,dc->vrd", plane, coul_cols, precision=lax.Precision.HIGHEST)
    screened = jnp.einsum("ab,vbc->vac", coul_rows, by_columns, precision=lax.Precision.HIGHEST)
    return screened
```

```python
import functools

import jax
import jax.numpy as jnp
from jax import lax
from jax.experimental import pallas as pl
from jax.experimental.pallas import tpu as pltpu
from jax.sharding import Mesh
from jax.sharding import PartitionSpec as P

SIDE = 256
Z, XH, Y, XL, CORE = "z", "x_hi", "y", "x_lo", "core"
CELL = (Y, XL, CORE)
ORB = (Z, XH)
CHIP = (Y, XL)
F32, BF16 = jnp.float32, jnp.bfloat16
HIGH = lax.Precision.HIGHEST
SWAP = ((0, 1), (1, 0))


def swapped(shard, axis):
    return lax.ppermute(shard, axis, SWAP)


def exchanged(parts, axes):
    return lax.all_to_all(parts, axes, split_axis=0, concat_axis=0, tiled=True)


def products(occ, basis, first, count):
    rows = [occ[first + n : first + n + 1, :] * basis for n in range(count)]
    return jnp.concatenate(rows, axis=0)


def project_kernel(occ_ref, basis_ref, pot_ref, far_ref, near_ref, *, group):
    step, half = pl.program_id(0), pl.num_programs(0) // 2
    blocks, count, width = occ_ref.shape
    parts = []
    for first in range(0, count, group):
        total = None
        for k in range(blocks):
            cut = slice(k * width, (k + 1) * width)
            pairs = products(occ_ref[k], basis_ref[:, cut], first, group)
            term = lax.dot_general(
                pot_ref[:, cut], pairs, (((1,), (1,)), ((), ())), preferred_element_type=F32
            )
            total = term if total is None else total + term
        parts.append(total)

    @pl.when(step < half)
    def _():
        for n, total in enumerate(parts):
            far_ref[n] = total

    @pl.when(step >= half)
    def _():
        for n, total in enumerate(parts):
            near_ref[n] = total


def project(occ, basis, pot, group, per_step):
    blocks, slots, width = occ.shape
    rows, points = basis.shape
    nv = pot.shape[0]
    steps = slots // per_step
    half = steps // 2
    out_count = per_step // group
    lanes = group * rows
    out = jax.ShapeDtypeStruct((slots // 2 // group, nv, lanes), F32)
    return pl.pallas_call(
        functools.partial(project_kernel, group=group),
        grid=(steps,),
        in_specs=[
            pl.BlockSpec((blocks, per_step, width), lambda t: (0, t, 0)),
            pl.BlockSpec((rows, points), lambda t: (0, 0)),
            pl.BlockSpec((nv, points), lambda t: (0, 0)),
        ],
        out_specs=[
            pl.BlockSpec((out_count, nv, lanes), lambda t: (jnp.minimum(t, half - 1), 0, 0)),
            pl.BlockSpec((out_count, nv, lanes), lambda t: (jnp.maximum(t - half, 0), 0, 0)),
        ],
        out_shape=[out, out],
        cost_estimate=pl.CostEstimate(
            flops=2 * slots * rows * points * nv, bytes_accessed=10_000_000, transcendentals=0
        ),
        name="project",
    )(occ, basis, pot)


def respond_kernel(occ_ref, basis_ref, far_ref, near_ref, out_ref, *, group):
    blocks, nv, lanes = far_ref.shape
    total = None
    for h, ref in enumerate((far_ref, near_ref)):
        for b in range(blocks):
            pairs = products(occ_ref[0], basis_ref[...], (h * blocks + b) * group, group)
            term = jnp.dot(ref[b], pairs, preferred_element_type=F32)
            total = term if total is None else total + term
    owners, lines, per_owner, side = out_ref.shape
    for n in range(owners):
        for r in range(lines):
            piece = total[n * per_owner : (n + 1) * per_owner, r * side : (r + 1) * side]
            out_ref[n, r] = piece.astype(out_ref.dtype)


def respond(occ, basis, far, near, group, owners):
    blocks, slots, width = occ.shape
    rows, points = basis.shape
    count, nv, lanes = far.shape
    lines = width // SIDE
    return pl.pallas_call(
        functools.partial(respond_kernel, group=group),
        grid=(blocks,),
        in_specs=[
            pl.BlockSpec((1, slots, width), lambda k: (k, 0, 0)),
            pl.BlockSpec((rows, width), lambda k: (0, k)),
            pl.BlockSpec((count, nv, lanes), lambda k: (0, 0, 0)),
            pl.BlockSpec((count, nv, lanes), lambda k: (0, 0, 0)),
        ],
        out_specs=pl.BlockSpec((owners, lines, nv // owners, SIDE), lambda k: (0, k, 0, 0)),
        out_shape=jax.ShapeDtypeStruct((owners, points // SIDE, nv // owners, SIDE), BF16),
        cost_estimate=pl.CostEstimate(
            flops=2 * slots * rows * points * nv, bytes_accessed=6_000_000, transcendentals=0
        ),
        name="respond",
    )(occ, basis, far, near)


def columns_kernel(plane_ref, cols_ref, out_ref):
    nv, lines, side = plane_ref.shape
    mixed = lax.dot_general(
        plane_ref[...].reshape(nv * lines, side),
        cols_ref[...],
        (((1,), (1,)), ((), ())),
        precision=HIGH,
        preferred_element_type=F32,
    ).reshape(nv, lines, side)
    per_dest = out_ref.shape[2] // 128
    for u in range(nv * side // 128):
        piece = mixed[u // 2, :, (u % 2) * 128 : (u % 2 + 1) * 128]
        at = u % per_dest * 128
        out_ref[u // per_dest, :, at : at + 128] = piece.astype(out_ref.dtype)


def rows_kernel(near_ref, far_ref, mix_near_ref, mix_far_ref, out_ref):
    chips, lines, width = near_ref.shape
    total = None
    for ref, mix in ((near_ref, mix_near_ref), (far_ref, mix_far_ref)):
        block = ref[...].astype(F32).reshape(chips * lines, width)
        term = jnp.dot(mix[...], block, precision=HIGH, preferred_element_type=F32)
        total = term if total is None else total + term
    out_ref[...] = total.reshape(chips, lines, width).astype(out_ref.dtype)


def final_kernel(parts_ref, out_ref):
    nv, lines, side = out_ref.shape
    per_dest = parts_ref.shape[2] // 128
    for u in range(nv * side // 128):
        at = u % per_dest * 128
        piece = parts_ref[u // per_dest, :, at : at + 128]
        out_ref[u // 2, :, (u % 2) * 128 : (u % 2 + 1) * 128] = piece.astype(F32)


def small_call(kernel, out, *args):
    return pl.pallas_call(kernel, out_shape=out, name=kernel.__name__)(*args)


def body(potentials, orbitals, levels, occ_index, coul_rows, coul_cols):
    nv, points = potentials.shape
    mine = orbitals.shape[0]
    norb, nocc = levels.shape[0], occ_index.shape[0]
    nz, nx, ny, nl, nc = (lax.axis_size(a) for a in (Z, XH, Y, XL, CORE))
    z, xh, y, xl, core = (lax.axis_index(a) for a in (Z, XH, Y, XL, CORE))
    chips = ny * nl
    chip = y * nl + xl
    width = points // nz
    slots = nocc // nx
    group = slots // (nc * chips)
    volume = points * chips * nc

    basis = jnp.concatenate([orbitals, swapped(orbitals, XH)], axis=0)

    by_points = exchanged(jnp.moveaxis(orbitals.reshape(mine, nz, width), 1, 0), Z)
    by_points = by_points.reshape(nz * mine, width)
    held = jnp.arange(nz * mine, dtype=jnp.int32)
    held = (held // mine * nx + xh) * mine + held % mine
    place = jnp.arange(slots, dtype=jnp.int32)
    place = (place + (1 - core) * (slots // 2)) % slots
    kept_occ = occ_index[xh * slots + place]
    sent_occ = occ_index[(1 - xh) * slots + place]

    def selected(wanted):
        chosen = (wanted[:, None] == held[None, :]).astype(BF16)
        return jnp.dot(chosen, by_points, preferred_element_type=F32).astype(BF16)

    occ_part = selected(kept_occ) + swapped(selected(sent_occ), XH)
    occ = exchanged(jnp.broadcast_to(occ_part, (nz, *occ_part.shape)), Z)

    far, near = project(occ, basis, potentials, group, 16)
    summed = (near + swapped(far, CORE)).astype(BF16)
    arrived = exchanged(summed, CHIP)
    intersection = jnp.sum(arrived.astype(F32), axis=0)

    labels = jnp.arange(norb, dtype=jnp.int32)
    empty = 1.0 - jnp.any(occ_index[:, None] == labels[None, :], axis=0).astype(F32)
    lane = jnp.arange(group * nx * mine, dtype=jnp.int32)
    slot = xh * slots + core * (slots // 2) + chip * group + lane // (nx * mine)
    partner = lane % (nx * mine) // mine
    other = (z * nx + (xh + partner) % nx) * mine + lane % mine
    weight = -2.0 * empty[other] / (levels[occ_index[slot]] + levels[other]) / volume
    guess = (intersection * weight[None, :]).astype(BF16)

    near_guess = exchanged(jnp.broadcast_to(guess, (chips, *guess.shape)), CHIP)
    far_guess = swapped(near_guess, CORE)
    response = respond(occ, basis, far_guess, near_guess, group, nz)

    owned = jnp.sum(exchanged(response, Z).astype(F32), axis=0)
    count = nv // (nz * nx)
    low, high = owned[:, :count], owned[:, count:]
    kept = jnp.where(xh == 0, low, high)
    sent = jnp.where(xh == 0, high, low).astype(BF16)
    plane = jnp.swapaxes(kept + swapped(sent, XH).astype(F32), 0, 1)

    lines = points // SIDE
    out = jax.ShapeDtypeStruct((chips, lines, count * SIDE // chips), BF16)
    columns = small_call(columns_kernel, out, plane, coul_cols)
    near_cols = exchanged(columns, CHIP)
    far_cols = swapped(near_cols, CORE)
    mix = coul_rows.reshape(chips, nc, lines, chips, nc, lines)
    mix = lax.dynamic_index_in_dim(mix, core, 1, keepdims=False)
    mix_near = lax.dynamic_index_in_dim(mix, core, 3, keepdims=False)
    mix_far = lax.dynamic_index_in_dim(mix, 1 - core, 3, keepdims=False)
    side = chips * lines
    mixed = small_call(
        rows_kernel,
        jax.ShapeDtypeStruct(columns.shape, F32),
        near_cols,
        far_cols,
        mix_near.reshape(side, side),
        mix_far.reshape(side, side),
    )
    parts = exchanged(mixed, CHIP)
    return small_call(final_kernel, jax.ShapeDtypeStruct((count, lines, SIDE), F32), parts)


def solution(mesh):
    torus = Mesh(mesh.devices.reshape(8, 2, 4, 2, 2), (Z, XH, Y, XL, CORE))
    return jax.shard_map(
        body,
        mesh=torus,
        in_specs=(P(None, CELL), P(ORB, CELL), P(), P(), P(), P()),
        out_specs=P(ORB, CELL, None),
        check_vma=False,
    )
```

```python
import functools

import jax
import jax.numpy as jnp
from jax import lax
from jax.experimental import pallas as pl
from jax.experimental.pallas import tpu as pltpu
from jax.sharding import Mesh
from jax.sharding import PartitionSpec as P

SIDE = 256
Z, XH, Y, XL, CORE = "z", "x_hi", "y", "x_lo", "core"
CELL = (Y, XL, CORE)
ORB = (Z, XH)
CHIP = (Y, XL)
F32, BF16 = jnp.float32, jnp.bfloat16
HIGH = lax.Precision.HIGHEST
SWAP = ((0, 1), (1, 0))


def swapped(shard, axis):
    return lax.ppermute(shard, axis, SWAP)


def exchanged(parts, axes):
    return lax.all_to_all(parts, axes, split_axis=0, concat_axis=0, tiled=True)


def products(occ, basis, first, count):
    rows = [occ[first + n : first + n + 1, :] * basis for n in range(count)]
    return jnp.concatenate(rows, axis=0)


def project_kernel(occ_ref, basis_ref, pot_ref, *out_refs, group):
    blocks, count, width = occ_ref.shape
    for n in range(count // group):
        total = None
        for k in range(blocks):
            cut = slice(k * width, (k + 1) * width)
            pairs = products(occ_ref[k], basis_ref[:, cut], n * group, group)
            term = lax.dot_general(
                pot_ref[:, cut], pairs, (((1,), (1,)), ((), ())), preferred_element_type=F32
            )
            total = term if total is None else total + term
        first = 0
        for ref in out_refs:
            ref[n] = total[first : first + ref.shape[1]]
            first += ref.shape[1]


def project(occ, basis, pot, group, per_step, chunks):
    blocks, slots, width = occ.shape
    rows, points = basis.shape
    nv = pot.shape[0]
    out_count = per_step // group
    lanes = group * rows
    return pl.pallas_call(
        functools.partial(project_kernel, group=group),
        grid=(slots // per_step,),
        in_specs=[
            pl.BlockSpec((blocks, per_step, width), lambda t: (0, t, 0)),
            pl.BlockSpec((rows, points), lambda t: (0, 0)),
            pl.BlockSpec((nv, points), lambda t: (0, 0)),
        ],
        out_specs=[pl.BlockSpec((out_count, c, lanes), lambda t: (t, 0, 0)) for c in chunks],
        out_shape=[jax.ShapeDtypeStruct((slots // group, c, lanes), F32) for c in chunks],
        cost_estimate=pl.CostEstimate(
            flops=2 * slots * rows * points * nv, bytes_accessed=6_000_000, transcendentals=0
        ),
        name="project",
    )(occ, basis, pot)


def respond_kernel(far_occ, near_occ, basis_ref, far_ref, near_ref, sent_ref, kept_ref, *, group):
    total = None
    for occ_ref, ref in ((far_occ, far_ref), (near_occ, near_ref)):
        for b in range(ref.shape[0]):
            pairs = products(occ_ref[0], basis_ref[...], b * group, group)
            term = jnp.dot(ref[b], pairs, preferred_element_type=F32)
            total = term if total is None else total + term
    first = 0
    for ref in (sent_ref, kept_ref):
        owners, lines, per_owner, side = ref.shape
        for n in range(owners):
            for r in range(lines):
                piece = total[first : first + per_owner, r * side : (r + 1) * side]
                ref[n, r] = piece.astype(ref.dtype)
            first += per_owner


def respond(far_occ, near_occ, basis, far, near, group, owners):
    blocks, slots, width = far_occ.shape
    rows, points = basis.shape
    count, nv, lanes = far.shape
    lines = width // SIDE
    per_owner = nv // owners // 2
    dims = (owners, points // SIDE, per_owner, SIDE)
    occ_spec = pl.BlockSpec((1, slots, width), lambda k: (k, 0, 0))
    guess_spec = pl.BlockSpec((count, nv, lanes), lambda k: (0, 0, 0))
    out_spec = pl.BlockSpec((owners, lines, per_owner, SIDE), lambda k: (0, k, 0, 0))
    return pl.pallas_call(
        functools.partial(respond_kernel, group=group),
        grid=(blocks,),
        in_specs=[
            occ_spec,
            occ_spec,
            pl.BlockSpec((rows, width), lambda k: (0, k)),
            guess_spec,
            guess_spec,
        ],
        out_specs=[out_spec, out_spec],
        out_shape=[jax.ShapeDtypeStruct(dims, BF16), jax.ShapeDtypeStruct(dims, F32)],
        cost_estimate=pl.CostEstimate(
            flops=4 * slots * rows * points * nv, bytes_accessed=6_000_000, transcendentals=0
        ),
        name="respond",
    )(far_occ, near_occ, basis, far, near)


def columns_kernel(plane_ref, cols_ref, out_ref):
    count, lines, side = plane_ref.shape
    mixed = lax.dot_general(
        plane_ref[...].reshape(count * lines, side),
        cols_ref[...],
        (((1,), (1,)), ((), ())),
        precision=HIGH,
        preferred_element_type=F32,
    )
    out_ref[...] = mixed.reshape(count, lines, side).astype(out_ref.dtype)


def in_three(block):
    high = block.astype(BF16)
    rest = block - high.astype(F32)
    mid = rest.astype(BF16)
    low = (rest - mid.astype(F32)).astype(BF16)
    return high, mid, low


def rows_kernel(near_ref, far_ref, mix_near_ref, mix_far_ref, out_ref):
    chips, count, lines, side = near_ref.shape
    mixes = [jnp.concatenate(in_three(m[...]), axis=0) for m in (mix_near_ref, mix_far_ref)]
    for n in range(count):
        total = None
        for ref, mix in zip((near_ref, far_ref), mixes):
            block = jnp.concatenate([ref[k, n] for k in range(chips)], axis=0)
            term = jnp.dot(mix, block, preferred_element_type=F32)
            total = term if total is None else total + term
        out_ref[n] = total[:lines] + (total[lines : 2 * lines] + total[2 * lines :])


def small_call(kernel, out, *args):
    return pl.pallas_call(kernel, out_shape=out, name=kernel.__name__)(*args)


def body(potentials, orbitals, levels, occ_index, coul_rows, coul_cols):
    nv, points = potentials.shape
    mine = orbitals.shape[0]
    norb, nocc = levels.shape[0], occ_index.shape[0]
    nz, nx, ny, nl, nc = (lax.axis_size(a) for a in (Z, XH, Y, XL, CORE))
    z, xh, y, xl, core = (lax.axis_index(a) for a in (Z, XH, Y, XL, CORE))
    chips = ny * nl
    chip = y * nl + xl
    width = points // nz
    slots = nocc // nx
    half = slots // nc
    group = half // chips
    lines = points // SIDE
    volume = points * chips * nc
    per_owner = nv // (nz * nx)
    big = per_owner * 2 // 3
    sizes = (big, per_owner - big)

    partner = swapped(orbitals, XH)
    by_points = exchanged(jnp.moveaxis(orbitals.reshape(mine, nz, width), 1, 0), Z)
    by_points = by_points.reshape(nz * mine, width)
    held = jnp.arange(nz * mine, dtype=jnp.int32)
    held = (held // mine * nx + xh) * mine + held % mine

    def slots_of(side):
        parts = [
            lax.dynamic_slice_in_dim(occ_index, side * slots + c * half, half)
            for c in (1 - core, core)
        ]
        return jnp.concatenate(parts)

    def selected(wanted):
        chosen = (wanted[:, None] == held[None, :]).astype(BF16)
        return jnp.dot(chosen, by_points, preferred_element_type=F32).astype(BF16)

    occ_part = selected(slots_of(xh)) + swapped(selected(slots_of(1 - xh)), XH)

    def spread(part, axes, count):
        return exchanged(jnp.broadcast_to(part, (count, *part.shape)), axes)

    far_occ = spread(occ_part[:half], Z, nz)
    near_occ = spread(occ_part[half:], Z, nz)

    place = jnp.arange(nv, dtype=jnp.int32)
    sources, first = [], 0
    for size in sizes:
        n = jnp.arange(nx * nz * size, dtype=jnp.int32)
        side = (xh + 1 + n // (nz * size)) % nx
        owner = n // size % nz * nx + side
        sources.append(owner * per_owner + first + n % size)
        first += size
    order = (jnp.concatenate(sources)[:, None] == place[None, :]).astype(BF16)
    pot = jnp.dot(order, potentials, preferred_element_type=F32).astype(BF16)
    basis = jnp.concatenate([orbitals, partner], axis=0)

    labels = jnp.arange(norb, dtype=jnp.int32)
    empty = 1.0 - jnp.any(occ_index[:, None] == labels[None, :], axis=0).astype(F32)
    own_slots = lax.dynamic_slice_in_dim(
        occ_index, xh * slots + core * half + chip * group, group
    )
    own_levels = jnp.sum(
        jnp.where(own_slots[:, None] == labels[None, :], levels[None, :], 0.0), axis=1
    )

    def of_basis(values):
        starts = [(z * nx + side) * mine for side in (xh, 1 - xh)]
        return jnp.concatenate([lax.dynamic_slice_in_dim(values, s, mine) for s in starts])

    weight = -2.0 * of_basis(empty)[None, :] / (own_levels[:, None] + of_basis(levels)[None, :])
    weight = (weight / volume).reshape(1, group * nx * mine)

    my_rows = lax.dynamic_slice_in_dim(coul_rows, (chip * nc + core) * lines, lines)
    my_rows = my_rows.reshape(lines, chips, nc, lines)
    mixes = [
        lax.dynamic_index_in_dim(my_rows, c, 2, keepdims=False).reshape(lines, chips * lines)
        for c in (core, 1 - core)
    ]
    far_occ, pot, weight, mixes = lax.optimization_barrier((far_occ, pot, weight, mixes))

    chunk_rows = [nx * nz * size for size in sizes]
    per_step = min(half, 16)
    far = project(far_occ, basis, pot, group, per_step, chunk_rows)
    near = project(near_occ, basis, pot, group, per_step, chunk_rows)

    screened = []
    for far_part, near_part in zip(far, near):
        summed = (near_part + swapped(far_part, CORE)).astype(BF16)
        intersection = jnp.sum(exchanged(summed, CHIP).astype(F32), axis=0)
        guess = (intersection * weight).astype(BF16)
        near_guess = spread(guess, CHIP, chips)
        far_guess = swapped(near_guess, CORE)
        sent, kept = respond(far_occ, near_occ, basis, far_guess, near_guess, group, nz)
        part = (kept + swapped(sent, XH).astype(F32)).astype(BF16)
        plane = jnp.swapaxes(jnp.sum(exchanged(part, Z).astype(F32), axis=0), 0, 1)
        columns = small_call(
            columns_kernel, jax.ShapeDtypeStruct(plane.shape, BF16), plane, coul_cols
        )
        near_cols = spread(columns, CHIP, chips)
        far_cols = swapped(near_cols, CORE)
        out = jax.ShapeDtypeStruct(plane.shape, F32)
        screened.append(small_call(rows_kernel, out, near_cols, far_cols, *mixes))
    return jnp.concatenate(screened, axis=0)


def solution(mesh):
    torus = Mesh(mesh.devices.reshape(8, 2, 4, 2, 2), (Z, XH, Y, XL, CORE))
    return jax.shard_map(
        body,
        mesh=torus,
        in_specs=(P(None, CELL), P(ORB, CELL), P(), P(), P(), P()),
        out_specs=P(ORB, CELL, None),
        check_vma=False,
    )
```

```python
import functools

import jax
import jax.numpy as jnp
from jax import lax
from jax.experimental import pallas as pl
from jax.experimental.pallas import tpu as pltpu
from jax.sharding import Mesh
from jax.sharding import PartitionSpec as P

SIDE = 256
Z, XH, Y, XL, CORE = "z", "x_hi", "y", "x_lo", "core"
CELL = (Y, XL, CORE)
ORB = (Z, XH)
CHIP = (Y, XL)
F32, BF16 = jnp.float32, jnp.bfloat16
HIGH = lax.Precision.HIGHEST
SWAP = ((0, 1), (1, 0))
ROOM = pltpu.CompilerParams(vmem_limit_bytes=32 * 2**20)


def swapped(shard, axis):
    return lax.ppermute(shard, axis, SWAP)


def exchanged(parts, axes):
    return lax.all_to_all(parts, axes, split_axis=0, concat_axis=0, tiled=True)


def products(occ, basis, first, count):
    rows = [occ[first + n : first + n + 1, :] * basis for n in range(count)]
    return jnp.concatenate(rows, axis=0)


def project_kernel(occ_ref, basis_ref, pot_ref, far_ref, near_ref, *, group):
    step, half = pl.program_id(0), pl.num_programs(0) // 2
    blocks, count, width = occ_ref.shape
    parts = []
    for first in range(0, count, group):
        total = None
        for k in range(blocks):
            cut = slice(k * width, (k + 1) * width)
            pairs = products(occ_ref[k], basis_ref[:, cut], first, group)
            term = lax.dot_general(
                pot_ref[:, cut], pairs, (((1,), (1,)), ((), ())), preferred_element_type=F32
            )
            total = term if total is None else total + term
        parts.append(total)

    @pl.when(step < half)
    def _():
        for n, total in enumerate(parts):
            far_ref[n] = total

    @pl.when(step >= half)
    def _():
        for n, total in enumerate(parts):
            near_ref[n] = total


def project(occ, basis, pot, group, per_step):
    blocks, slots, width = occ.shape
    rows, points = basis.shape
    nv = pot.shape[0]
    steps = slots // per_step
    half = steps // 2
    out_count = per_step // group
    lanes = group * rows
    out = jax.ShapeDtypeStruct((slots // 2 // group, nv, lanes), F32)
    return pl.pallas_call(
        functools.partial(project_kernel, group=group),
        grid=(steps,),
        in_specs=[
            pl.BlockSpec((blocks, per_step, width), lambda t: (0, t, 0)),
            pl.BlockSpec((rows, points), lambda t: (0, 0)),
            pl.BlockSpec((nv, points), lambda t: (0, 0)),
        ],
        out_specs=[
            pl.BlockSpec((out_count, nv, lanes), lambda t: (jnp.minimum(t, half - 1), 0, 0)),
            pl.BlockSpec((out_count, nv, lanes), lambda t: (jnp.maximum(t - half, 0), 0, 0)),
        ],
        out_shape=[out, out],
        cost_estimate=pl.CostEstimate(
            flops=2 * slots * rows * points * nv, bytes_accessed=10_000_000, transcendentals=0
        ),
        compiler_params=ROOM,
        name="project",
    )(occ, basis, pot)


def respond_kernel(own_occ, other_occ, basis_ref, far_ref, near_ref, out_ref, *, group):
    blocks = far_ref.shape[0]
    total = None
    for p, occ_ref in enumerate((own_occ, other_occ)):
        for h, ref in enumerate((far_ref, near_ref)):
            for b in range(blocks):
                pairs = products(occ_ref[0], basis_ref[...], (h * blocks + b) * group, group)
                term = jnp.dot(ref[b, p], pairs, preferred_element_type=F32)
                total = term if total is None else total + term
    owners, count, side = out_ref.shape
    per_owner = total.shape[0] // owners
    for n in range(owners):
        rows = total[n * per_owner : (n + 1) * per_owner]
        lines = [rows[:, r * side : (r + 1) * side] for r in range(count // per_owner)]
        out_ref[n] = jnp.concatenate(lines, axis=0).astype(out_ref.dtype)


def respond(own_occ, other_occ, basis, far, near, group, owners):
    blocks, slots, width = own_occ.shape
    rows, points = basis.shape
    nv = far.shape[2]
    occ_spec = pl.BlockSpec((1, slots, width), lambda k: (k, 0, 0))
    guess_spec = pl.BlockSpec(far.shape, lambda k: (0, 0, 0, 0))
    lines = nv // owners * (width // SIDE)
    return pl.pallas_call(
        functools.partial(respond_kernel, group=group),
        grid=(blocks,),
        in_specs=[
            occ_spec,
            occ_spec,
            pl.BlockSpec((rows, width), lambda k: (0, k)),
            guess_spec,
            guess_spec,
        ],
        out_specs=pl.BlockSpec((owners, lines, SIDE), lambda k: (0, k, 0)),
        out_shape=jax.ShapeDtypeStruct((owners, blocks * lines, SIDE), BF16),
        cost_estimate=pl.CostEstimate(
            flops=4 * slots * rows * points * nv, bytes_accessed=6_000_000, transcendentals=0
        ),
        compiler_params=ROOM,
        name="respond",
    )(own_occ, other_occ, basis, far, near)


def columns_kernel(parts_ref, cols_ref, out_ref):
    sources, size, side = parts_ref.shape
    copies, count, lines, _ = out_ref.shape
    plane = parts_ref[0].astype(F32)
    for s in range(1, sources):
        plane = plane + parts_ref[s].astype(F32)
    mixed = lax.dot_general(
        plane, cols_ref[...], (((1,), (1,)), ((), ())), precision=HIGH, preferred_element_type=F32
    ).astype(BF16)
    row = lax.broadcasted_iota(jnp.int32, (size, size), 0)
    column = lax.broadcasted_iota(jnp.int32, (size, size), 1)
    source = row % lines * count + row // lines
    swap = jnp.where(source == column, 1.0, 0.0).astype(BF16)
    block = jnp.dot(swap, mixed, preferred_element_type=F32).astype(BF16)
    block = block.reshape(count, lines, side)
    for n in range(copies):
        out_ref[n] = block


def in_three(block):
    high = block.astype(BF16)
    rest = block - high.astype(F32)
    mid = rest.astype(BF16)
    low = (rest - mid.astype(F32)).astype(BF16)
    return high, mid, low


def rows_kernel(near_ref, far_ref, mix_near_ref, mix_far_ref, out_ref):
    chips, count, lines, _ = near_ref.shape
    mixes = [jnp.concatenate(in_three(m[...]), axis=0) for m in (mix_near_ref, mix_far_ref)]
    for n in range(count):
        total = None
        for ref, mix in zip((near_ref, far_ref), mixes):
            block = jnp.concatenate([ref[k, n] for k in range(chips)], axis=0)
            term = jnp.dot(mix, block, preferred_element_type=F32)
            total = term if total is None else total + term
        out_ref[n] = total[:lines] + (total[lines : 2 * lines] + total[2 * lines :])


def small_call(kernel, out, *args):
    return pl.pallas_call(kernel, out_shape=out, compiler_params=ROOM)(*args)


def body(potentials, orbitals, levels, occ_index, coul_rows, coul_cols):
    nv, points = potentials.shape
    mine = orbitals.shape[0]
    norb, nocc = levels.shape[0], occ_index.shape[0]
    nz, nx, ny, nl, nc = (lax.axis_size(a) for a in (Z, XH, Y, XL, CORE))
    z, xh, y, xl, core = (lax.axis_index(a) for a in (Z, XH, Y, XL, CORE))
    chips = ny * nl
    chip = y * nl + xl
    width = points // nz
    slots = nocc // nx
    half = slots // nc
    group = half // chips
    lines = points // SIDE
    volume = points * chips * nc
    per_owner = nv // (nz * nx)

    partner = swapped(orbitals, XH)
    by_points = exchanged(jnp.moveaxis(orbitals.reshape(mine, nz, width), 1, 0), Z)
    by_points = by_points.reshape(nz * mine, width)
    held = jnp.arange(nz * mine, dtype=jnp.int32)
    held = (held // mine * nx + xh) * mine + held % mine

    def slots_of(side):
        parts = [
            lax.dynamic_slice_in_dim(occ_index, side * slots + c * half, half)
            for c in (1 - core, core)
        ]
        return jnp.concatenate(parts)

    def selected(wanted):
        chosen = (wanted[:, None] == held[None, :]).astype(BF16)
        return jnp.dot(chosen, by_points, preferred_element_type=F32).astype(BF16)

    def spread(part, axes, count):
        return exchanged(jnp.broadcast_to(part, (count, *part.shape)), axes)

    occ_part = selected(slots_of(xh)) + swapped(selected(slots_of(1 - xh)), XH)
    occ = spread(occ_part, Z, nz)

    place = jnp.arange(nv, dtype=jnp.int32)
    side = (xh + 1 + place // (nz * per_owner)) % nx
    source = (place // per_owner % nz * nx + side) * per_owner + place % per_owner
    order = (source[:, None] == place[None, :]).astype(BF16)
    pot = jnp.dot(order, potentials, preferred_element_type=F32).astype(BF16)
    first = jnp.where(xh == 0, orbitals, partner)
    second = jnp.where(xh == 0, partner, orbitals)
    basis = jnp.concatenate([first, second], axis=0)

    labels = jnp.arange(norb, dtype=jnp.int32)
    empty = 1.0 - jnp.any(occ_index[:, None] == labels[None, :], axis=0).astype(F32)
    own_slots = lax.dynamic_slice_in_dim(
        occ_index, xh * slots + core * half + chip * group, group
    )
    own_levels = jnp.sum(
        jnp.where(own_slots[:, None] == labels[None, :], levels[None, :], 0.0), axis=1
    )

    def of_basis(values):
        return lax.dynamic_slice_in_dim(values, z * nx * mine, nx * mine)

    weight = -2.0 * of_basis(empty)[None, :] / (own_levels[:, None] + of_basis(levels)[None, :])
    weight = (weight / volume).reshape(1, group * nx * mine)

    my_rows = lax.dynamic_slice_in_dim(coul_rows, (chip * nc + core) * lines, lines)
    my_rows = my_rows.reshape(lines, chips, nc, lines)
    mixes = [
        lax.dynamic_index_in_dim(my_rows, c, 2, keepdims=False).reshape(lines, chips * lines)
        for c in (core, 1 - core)
    ]
    occ, pot, weight, mixes = lax.optimization_barrier((occ, pot, weight, mixes))

    other_occ = swapped(occ, XH)
    far, near = project(occ, basis, pot, group, 16)
    near, other_occ = lax.optimization_barrier((near, other_occ))
    summed = (near + swapped(far, CORE)).astype(BF16)
    intersection = jnp.sum(exchanged(summed, CHIP).astype(F32), axis=0)
    guess = (intersection * weight).astype(BF16)

    given, kept = guess[: nv // nx], guess[nv // nx :]
    guesses = jnp.stack([kept, swapped(given, XH)])
    near_guess = spread(guesses, CHIP, chips)
    far_guess = swapped(near_guess, CORE)
    response = respond(occ, other_occ, basis, far_guess, near_guess, group, nz)

    out = jax.ShapeDtypeStruct((chips, per_owner, lines, SIDE), BF16)
    columns = small_call(columns_kernel, out, exchanged(response, Z), coul_cols)
    near_cols = exchanged(columns, CHIP)
    far_cols = swapped(near_cols, CORE)
    out = jax.ShapeDtypeStruct((per_owner, lines, SIDE), F32)
    return small_call(rows_kernel, out, near_cols, far_cols, *mixes)


def solution(mesh):
    torus = Mesh(mesh.devices.reshape(8, 2, 4, 2, 2), (Z, XH, Y, XL, CORE))
    return jax.shard_map(
        body,
        mesh=torus,
        in_specs=(P(None, CELL), P(ORB, CELL), P(), P(), P(), P()),
        out_specs=P(ORB, CELL, None),
        check_vma=False,
    )
```

```python
import functools

import jax
import jax.numpy as jnp
from jax import lax
from jax.experimental import pallas as pl
from jax.experimental.pallas import tpu as pltpu
from jax.sharding import Mesh
from jax.sharding import PartitionSpec as P

SIDE = 256
Z, XH, Y, XL, CORE = "z", "x_hi", "y", "x_lo", "core"
CELL = (Y, XL, CORE)
ORB = (Z, XH)
CHIP = (Y, XL)
F32, BF16 = jnp.float32, jnp.bfloat16
HIGH = lax.Precision.HIGHEST
SWAP = ((0, 1), (1, 0))
ROOM = pltpu.CompilerParams(vmem_limit_bytes=20 * 2**20)


def swapped(shard, axis):
    return lax.ppermute(shard, axis, SWAP)


def exchanged(parts, axes):
    return lax.all_to_all(parts, axes, split_axis=0, concat_axis=0, tiled=True)


def split_kernel(rows_ref, out_ref):
    width = out_ref.shape[2]
    for k in range(out_ref.shape[0]):
        out_ref[k] = rows_ref[:, k * width : (k + 1) * width]


def pick_kernel(wanted_ref, rows_ref, out_ref):
    count, stored = wanted_ref.shape[0], rows_ref.shape[0]
    label = lax.broadcasted_iota(jnp.int32, (count, stored), 1)
    chosen = jnp.where(wanted_ref[...] == label, 1.0, 0.0).astype(BF16)
    picked = jnp.dot(chosen, rows_ref[...], preferred_element_type=F32).astype(BF16)
    slots = out_ref.shape[1]
    for k in range(out_ref.shape[0]):
        n = k % (count // slots)
        out_ref[k] = picked[n * slots : (n + 1) * slots]


def join_kernel(near_ref, far_ref, out_ref):
    out_ref[...] = (near_ref[...] + far_ref[...]).astype(out_ref.dtype)


def products(occ, places, parts):
    return jnp.concatenate([occ[n : n + 1, :] * part for n in places for part in parts], axis=0)


def project_kernel(occ_ref, first_ref, second_ref, pot_ref, out_ref, *, group):
    blocks, count, width = occ_ref.shape
    for n in range(count // group):
        total = None
        for k in range(blocks):
            cut = slice(k * width, (k + 1) * width)
            parts = (first_ref[:, cut], second_ref[:, cut])
            pairs = products(occ_ref[k], range(n * group, (n + 1) * group), parts)
            term = lax.dot_general(
                pot_ref[:, cut], pairs, (((1,), (1,)), ((), ())), preferred_element_type=F32
            )
            total = term if total is None else total + term
        out_ref[n] = total


def project(occ, start, steps, first, second, pot, group):
    blocks, _, width = occ.shape
    rows, points = first.shape
    nv = pot.shape[0]
    per_step = 16
    outs, lanes = per_step // group, 2 * group * rows
    row_spec = pl.BlockSpec((rows, points), lambda t: (0, 0))
    return pl.pallas_call(
        functools.partial(project_kernel, group=group),
        grid=(steps,),
        in_specs=[
            pl.BlockSpec((blocks, per_step, width), lambda t: (0, start + t, 0)),
            row_spec,
            row_spec,
            pl.BlockSpec((nv, points), lambda t: (0, 0)),
        ],
        out_specs=pl.BlockSpec((outs, nv, lanes), lambda t: (t, 0, 0)),
        out_shape=jax.ShapeDtypeStruct((outs * steps, nv, lanes), F32),
        cost_estimate=pl.CostEstimate(
            flops=4 * steps * per_step * rows * points * nv,
            bytes_accessed=4_000_000,
            transcendentals=0,
        ),
        compiler_params=ROOM,
        name="project",
    )(occ, first, second, pot)


def respond_kernel(own_occ, other_occ, first_ref, second_ref, far_ref, near_ref, out_ref, *, group):
    blocks, _, nv, _ = far_ref.shape
    owners, _, side = out_ref.shape
    per_owner = nv // owners
    lines = []
    for r in range(own_occ.shape[0]):
        cut = slice(r * side, (r + 1) * side)
        parts = (first_ref[:, cut], second_ref[:, cut])
        total = None
        for p, occ_ref in enumerate((own_occ, other_occ)):
            for h, ref in enumerate((far_ref, near_ref)):
                for b in range(blocks):
                    base = (h * blocks + b) * group
                    pairs = products(occ_ref[r], range(base, base + group), parts)
                    term = jnp.dot(ref[b, p], pairs, preferred_element_type=F32)
                    total = term if total is None else total + term
        lines.append(total)
    for n in range(owners):
        rows = [line[n * per_owner : (n + 1) * per_owner] for line in lines]
        out_ref[n] = jnp.concatenate(rows, axis=0).astype(out_ref.dtype)


def respond(own_occ, other_occ, start, steps, first, second, far, near, group, owners):
    _, slots, width = own_occ.shape
    rows, _ = first.shape
    nv = far.shape[2]
    occ_spec = pl.BlockSpec((2, slots, width), lambda k: (start + k, 0, 0))
    row_spec = pl.BlockSpec((rows, 2 * width), lambda k: (0, start + k))
    guess_spec = pl.BlockSpec(far.shape, lambda k: (0, 0, 0, 0))
    lines = 2 * nv // owners
    return pl.pallas_call(
        functools.partial(respond_kernel, group=group),
        grid=(steps,),
        in_specs=[occ_spec, occ_spec, row_spec, row_spec, guess_spec, guess_spec],
        out_specs=pl.BlockSpec((owners, lines, SIDE), lambda k: (0, k, 0)),
        out_shape=jax.ShapeDtypeStruct((owners, steps * lines, SIDE), BF16),
        cost_estimate=pl.CostEstimate(
            flops=16 * slots * rows * width * steps * nv,
            bytes_accessed=3_000_000,
            transcendentals=0,
        ),
        compiler_params=ROOM,
        name="respond",
    )(own_occ, other_occ, first, second, far, near)


def columns_kernel(top_ref, bottom_ref, cols_ref, out_ref):
    copies, count, lines, side = out_ref.shape
    size = count * lines
    planes = []
    for ref in (top_ref, bottom_ref):
        plane = ref[0].astype(F32)
        for s in range(1, ref.shape[0]):
            plane = plane + ref[s].astype(F32)
        planes.append(plane)
    plane = jnp.concatenate(planes, axis=0)
    mixed = lax.dot_general(
        plane, cols_ref[...], (((1,), (1,)), ((), ())), precision=HIGH, preferred_element_type=F32
    ).astype(BF16)
    row = lax.broadcasted_iota(jnp.int32, (size, size), 0)
    column = lax.broadcasted_iota(jnp.int32, (size, size), 1)
    source = row % lines * count + row // lines
    swap = jnp.where(source == column, 1.0, 0.0).astype(BF16)
    block = jnp.dot(swap, mixed, preferred_element_type=F32).astype(BF16)
    block = block.reshape(count, lines, side)
    for n in range(copies):
        out_ref[n] = block


def in_three(block):
    high = block.astype(BF16)
    rest = block - high.astype(F32)
    mid = rest.astype(BF16)
    low = (rest - mid.astype(F32)).astype(BF16)
    return high, mid, low


def rows_kernel(near_ref, far_ref, mix_near_ref, mix_far_ref, out_ref):
    chips, count, lines, _ = near_ref.shape
    mixes = [jnp.concatenate(in_three(m[...]), axis=0) for m in (mix_near_ref, mix_far_ref)]
    for n in range(count):
        total = None
        for ref, mix in zip((near_ref, far_ref), mixes):
            block = jnp.concatenate([ref[k, n] for k in range(chips)], axis=0)
            term = jnp.dot(mix, block, preferred_element_type=F32)
            total = term if total is None else total + term
        out_ref[n] = total[:lines] + (total[lines : 2 * lines] + total[2 * lines :])


def small_call(kernel, out, *args):
    return pl.pallas_call(kernel, out_shape=out, compiler_params=ROOM)(*args)


def body(potentials, orbitals, levels, occ_index, coul_rows, coul_cols):
    nv, points = potentials.shape
    mine = orbitals.shape[0]
    norb, nocc = levels.shape[0], occ_index.shape[0]
    nz, nx, ny, nl, nc = (lax.axis_size(a) for a in (Z, XH, Y, XL, CORE))
    z, xh, y, xl, core = (lax.axis_index(a) for a in (Z, XH, Y, XL, CORE))
    chips = ny * nl
    chip = y * nl + xl
    width = points // (nz * nx)
    slots = nocc // nx
    half = slots // nc
    group = half // chips
    lines = points // SIDE
    volume = points * chips * nc
    per_owner = nv // (nz * nx)

    blocks = jax.ShapeDtypeStruct((nz * nx, mine, width), BF16)
    by_points = exchanged(small_call(split_kernel, blocks, orbitals), ORB)
    partner = swapped(orbitals, XH)

    def part_of(values, start, count):
        return lax.dynamic_slice_in_dim(values, start, count)

    starts = [s * slots + c * half for s in range(nx) for c in (1 - core, core)]
    wanted = jnp.concatenate([part_of(occ_index, s, half) for s in starts])[:, None]
    copies = jax.ShapeDtypeStruct((nz * nx, slots, width), BF16)
    spread = small_call(pick_kernel, copies, wanted, by_points.reshape(norb, width))
    occ = exchanged(spread, ORB)

    place = jnp.arange(nv, dtype=jnp.int32)
    side = (xh + 1 + place // (nz * per_owner)) % nx
    source = (place // per_owner % nz * nx + side) * per_owner + place % per_owner
    order = (source[:, None] == place[None, :]).astype(BF16)
    pot = jnp.dot(order, potentials, preferred_element_type=F32).astype(BF16)
    first = jnp.where(xh == 0, orbitals, partner)
    second = jnp.where(xh == 0, partner, orbitals)

    labels = jnp.arange(norb, dtype=jnp.int32)
    empty = 1.0 - jnp.any(occ_index[:, None] == labels[None, :], axis=0).astype(F32)
    own_slots = part_of(occ_index, xh * slots + core * half + chip * group, group)
    own_levels = jnp.sum(
        jnp.where(own_slots[:, None] == labels[None, :], levels[None, :], 0.0), axis=1
    )
    stored = z * nx * mine
    basis_empty = part_of(empty, stored, nx * mine)
    basis_levels = part_of(levels, stored, nx * mine)
    weight = -2.0 * basis_empty[None, :] / (own_levels[:, None] + basis_levels[None, :])
    weight = (weight / volume).reshape(1, group * nx * mine)

    my_rows = part_of(coul_rows, (chip * nc + core) * lines, lines)
    my_rows = my_rows.reshape(lines, chips, nc, lines)
    mixes = [
        lax.dynamic_index_in_dim(my_rows, c, 2, keepdims=False).reshape(lines, chips * lines)
        for c in (core, 1 - core)
    ]
    held_back = (occ, pot, first, second, weight, mixes)
    occ, pot, first, second, weight, mixes = lax.optimization_barrier(held_back)

    other_occ = swapped(occ, XH)
    rest = (first, second, pot, group)
    far = project(occ, 0, half // 16, *rest)
    far = swapped(far, CORE)
    near = project(occ, half // 16, half // 16, *rest)
    near, other_occ = lax.optimization_barrier((near, other_occ))
    summed = small_call(join_kernel, jax.ShapeDtypeStruct(near.shape, BF16), near, far)
    intersection = jnp.sum(exchanged(summed, CHIP).astype(F32), axis=0)
    guess = (intersection * weight).astype(BF16)

    given, kept = guess[: nv // nx], guess[nv // nx :]
    guesses = jnp.stack([kept, swapped(given, XH)])
    near_guess = exchanged(jnp.broadcast_to(guesses, (chips, *guesses.shape)), CHIP)
    far_guess = swapped(near_guess, CORE)
    parts = []
    for n in range(2):
        response = respond(
            occ, other_occ, n * lines // 4, lines // 4, first, second, far_guess, near_guess,
            group, nz,
        )
        parts.append(exchanged(response, Z))

    out = jax.ShapeDtypeStruct((chips, per_owner, lines, SIDE), BF16)
    columns = small_call(columns_kernel, out, *parts, coul_cols)
    near_cols = exchanged(columns, CHIP)
    far_cols = swapped(near_cols, CORE)
    out = jax.ShapeDtypeStruct((per_owner, lines, SIDE), F32)
    return small_call(rows_kernel, out, near_cols, far_cols, *mixes)


def solution(mesh):
    torus = Mesh(mesh.devices.reshape(8, 2, 4, 2, 2), (Z, XH, Y, XL, CORE))
    return jax.shard_map(
        body,
        mesh=torus,
        in_specs=(P(None, CELL), P(ORB, CELL), P(), P(), P(), P()),
        out_specs=P(ORB, CELL, None),
        check_vma=False,
    )
```

```python
import functools

import jax
import jax.numpy as jnp
from jax import lax
from jax.experimental import pallas as pl
from jax.experimental.pallas import tpu as pltpu
from jax.sharding import Mesh
from jax.sharding import PartitionSpec as P

SIDE = 256
Z, XH, Y, XL, CORE = "z", "x_hi", "y", "x_lo", "core"
CELL = (Y, XL, CORE)
ORB = (Z, XH)
CHIP = (Y, XL)
F32, BF16 = jnp.float32, jnp.bfloat16
HIGH = lax.Precision.HIGHEST
SWAP = ((0, 1), (1, 0))
ROOM = pltpu.CompilerParams(vmem_limit_bytes=20 * 2**20)


def swapped(shard, axis):
    return lax.ppermute(shard, axis, SWAP)


def exchanged(parts, axes):
    return lax.all_to_all(parts, axes, split_axis=0, concat_axis=0, tiled=True)


def split_kernel(rows_ref, out_ref):
    width = out_ref.shape[2]
    for k in range(out_ref.shape[0]):
        out_ref[k] = rows_ref[:, k * width : (k + 1) * width]


def pick_kernel(wanted_ref, rows_ref, out_ref):
    count, stored = wanted_ref.shape[0], rows_ref.shape[0]
    label = lax.broadcasted_iota(jnp.int32, (count, stored), 1)
    chosen = jnp.where(wanted_ref[...] == label, 1.0, 0.0).astype(BF16)
    picked = jnp.dot(chosen, rows_ref[...], preferred_element_type=F32).astype(BF16)
    slots = out_ref.shape[1]
    for k in range(out_ref.shape[0]):
        n = k % (count // slots)
        out_ref[k] = picked[n * slots : (n + 1) * slots]


def order_kernel(source_ref, rows_ref, out_ref):
    count = source_ref.shape[0]
    label = lax.broadcasted_iota(jnp.int32, (count, count), 1)
    order = jnp.where(source_ref[...] == label, 1.0, 0.0).astype(BF16)
    out_ref[...] = jnp.dot(order, rows_ref[...], preferred_element_type=F32).astype(BF16)


def join_kernel(near_ref, far_ref, out_ref):
    out_ref[...] = (near_ref[...] + far_ref[...]).astype(out_ref.dtype)


def products(occ, places, parts):
    return jnp.concatenate([occ[n : n + 1, :] * part for n in places for part in parts], axis=0)


def project_kernel(occ_ref, first_ref, second_ref, pot_ref, out_ref, *, group):
    blocks, count, width = occ_ref.shape
    for n in range(count // group):
        total = None
        for k in range(blocks):
            cut = slice(k * width, (k + 1) * width)
            parts = (first_ref[:, cut], second_ref[:, cut])
            pairs = products(occ_ref[k], range(n * group, (n + 1) * group), parts)
            term = lax.dot_general(
                pot_ref[:, cut], pairs, (((1,), (1,)), ((), ())), preferred_element_type=F32
            )
            total = term if total is None else total + term
        out_ref[n] = total


def project(occ, start, first, second, pot, group):
    blocks, slots, width = occ.shape
    slots //= 2
    rows, points = first.shape
    nv = pot.shape[0]
    per_step = 16
    steps = slots // per_step
    start *= steps
    outs, lanes = per_step // group, 2 * group * rows
    row_spec = pl.BlockSpec((rows, points), lambda t: (0, 0))
    return pl.pallas_call(
        functools.partial(project_kernel, group=group),
        grid=(steps,),
        in_specs=[
            pl.BlockSpec((blocks, per_step, width), lambda t: (0, start + t, 0)),
            row_spec,
            row_spec,
            pl.BlockSpec((nv, points), lambda t: (0, 0)),
        ],
        out_specs=pl.BlockSpec((outs, nv, lanes), lambda t: (t, 0, 0)),
        out_shape=jax.ShapeDtypeStruct((outs * steps, nv, lanes), F32),
        cost_estimate=pl.CostEstimate(
            flops=4 * steps * per_step * rows * points * nv,
            bytes_accessed=4_000_000,
            transcendentals=0,
        ),
        compiler_params=ROOM,
        name="project",
    )(occ, first, second, pot)


def respond_kernel(*refs, group):
    *occ_refs, first_ref, second_ref, far_ref, near_ref, out_ref = refs
    blocks, _, nv, _ = far_ref.shape
    owners, _, side = out_ref.shape
    per_owner = nv // owners
    lines = []
    for r in range(occ_refs[0].shape[0]):
        cut = slice(r * side, (r + 1) * side)
        parts = (first_ref[:, cut], second_ref[:, cut])
        total = None
        for p, occ_ref in enumerate(occ_refs):
            for h, ref in enumerate((far_ref, near_ref)):
                for b in range(blocks):
                    base = (h * blocks + b) * group
                    places = range(base, base + group)
                    pairs = products(occ_ref[r], places, parts[:: 1 - 2 * p])
                    term = jnp.dot(ref[b, p], pairs, preferred_element_type=F32)
                    total = term if total is None else total + term
        lines.append(total)
    for n in range(owners):
        rows = [line[n * per_owner : (n + 1) * per_owner] for line in lines]
        out_ref[n] = jnp.concatenate(rows, axis=0).astype(out_ref.dtype)


def respond(occs, first, second, far, near, group, owners):
    count, slots, width = occs[0].shape
    rows, points = first.shape
    nv = far.shape[2]
    steps = count // 2
    occ_spec = pl.BlockSpec((2, slots, width), lambda k: (k, 0, 0))
    row_spec = pl.BlockSpec((rows, 2 * width), lambda k: (0, k))
    guess_spec = pl.BlockSpec(far.shape, lambda k: (0, 0, 0, 0))
    lines = 2 * nv // owners
    return pl.pallas_call(
        functools.partial(respond_kernel, group=group),
        grid=(steps,),
        in_specs=[occ_spec] * len(occs) + [row_spec, row_spec, guess_spec, guess_spec],
        out_specs=pl.BlockSpec((owners, lines, SIDE), lambda k: (0, k, 0)),
        out_shape=jax.ShapeDtypeStruct((owners, steps * lines, SIDE), BF16),
        cost_estimate=pl.CostEstimate(
            flops=4 * len(occs) * slots * rows * points * nv,
            bytes_accessed=6_000_000,
            transcendentals=0,
        ),
        compiler_params=ROOM,
        name="respond",
    )(*occs, first, second, far, near)


def columns_kernel(parts_ref, cols_ref, out_ref):
    copies, count, lines, side = out_ref.shape
    size = count * lines
    plane = parts_ref[0].astype(F32)
    for s in range(1, parts_ref.shape[0]):
        plane = plane + parts_ref[s].astype(F32)
    mixed = lax.dot_general(
        plane, cols_ref[...], (((1,), (1,)), ((), ())), precision=HIGH, preferred_element_type=F32
    ).astype(BF16)
    row = lax.broadcasted_iota(jnp.int32, (size, size), 0)
    column = lax.broadcasted_iota(jnp.int32, (size, size), 1)
    source = row % lines * count + row // lines
    swap = jnp.where(source == column, 1.0, 0.0).astype(BF16)
    block = jnp.dot(swap, mixed, preferred_element_type=F32).astype(BF16)
    block = block.reshape(count, lines, side)
    for n in range(copies):
        out_ref[n] = block


def in_three(block):
    high = block.astype(BF16)
    rest = block - high.astype(F32)
    mid = rest.astype(BF16)
    low = (rest - mid.astype(F32)).astype(BF16)
    return high, mid, low


def rows_kernel(near_ref, far_ref, mix_near_ref, mix_far_ref, out_ref):
    chips, count, lines, _ = near_ref.shape
    mixes = [jnp.concatenate(in_three(m[...]), axis=0) for m in (mix_near_ref, mix_far_ref)]
    for n in range(count):
        total = None
        for ref, mix in zip((near_ref, far_ref), mixes):
            block = jnp.concatenate([ref[k, n] for k in range(chips)], axis=0)
            term = jnp.dot(mix, block, preferred_element_type=F32)
            total = term if total is None else total + term
        out_ref[n] = total[:lines] + (total[lines : 2 * lines] + total[2 * lines :])


def small_call(kernel, out, *args):
    return pl.pallas_call(kernel, out_shape=out, compiler_params=ROOM)(*args)


def body(potentials, orbitals, levels, occ_index, coul_rows, coul_cols):
    nv, points = potentials.shape
    mine = orbitals.shape[0]
    norb, nocc = levels.shape[0], occ_index.shape[0]
    nz, nx, ny, nl, nc = (lax.axis_size(a) for a in (Z, XH, Y, XL, CORE))
    z, xh, y, xl, core = (lax.axis_index(a) for a in (Z, XH, Y, XL, CORE))
    chips = ny * nl
    chip = y * nl + xl
    width = points // (nz * nx)
    slots = nocc // nx
    half = slots // nc
    group = half // chips
    lines = points // SIDE
    volume = points * chips * nc
    per_owner = nv // (nz * nx)

    blocks = jax.ShapeDtypeStruct((nz * nx, mine, width), BF16)
    partner = swapped(orbitals, XH)
    by_points = exchanged(small_call(split_kernel, blocks, orbitals), ORB)

    def part_of(values, start, count):
        return lax.dynamic_slice_in_dim(values, start, count)

    starts = [s * slots + c * half for s in range(nx) for c in (1 - core, core)]
    wanted = jnp.concatenate([part_of(occ_index, s, half) for s in starts])[:, None]
    copies = jax.ShapeDtypeStruct((nz * nx, slots, width), BF16)
    spread = small_call(pick_kernel, copies, wanted, by_points.reshape(norb, width))
    occ = exchanged(spread, ORB)

    place = jnp.arange(nv, dtype=jnp.int32)
    side = (xh + 1 + place // (nz * per_owner)) % nx
    source = (place // per_owner % nz * nx + side) * per_owner + place % per_owner
    out = jax.ShapeDtypeStruct(potentials.shape, BF16)
    pot = small_call(order_kernel, out, source[:, None], potentials)

    labels = jnp.arange(norb, dtype=jnp.int32)
    empty = 1.0 - jnp.any(occ_index[:, None] == labels[None, :], axis=0).astype(F32)
    own_slots = part_of(occ_index, xh * slots + core * half + chip * group, group)
    own_levels = jnp.sum(
        jnp.where(own_slots[:, None] == labels[None, :], levels[None, :], 0.0), axis=1
    )
    stored = [(z * nx + n) * mine for n in (xh, 1 - xh)]
    basis_empty = jnp.concatenate([part_of(empty, n, mine) for n in stored])
    basis_levels = jnp.concatenate([part_of(levels, n, mine) for n in stored])
    weight = -2.0 * basis_empty[None, :] / (own_levels[:, None] + basis_levels[None, :])
    weight = (weight / volume).reshape(1, group * nx * mine)

    my_rows = part_of(coul_rows, (chip * nc + core) * lines, lines)
    my_rows = my_rows.reshape(lines, chips, nc, lines)
    mixes = [
        lax.dynamic_index_in_dim(my_rows, c, 2, keepdims=False).reshape(lines, chips * lines)
        for c in (core, 1 - core)
    ]
    occ, pot, weight, mixes = lax.optimization_barrier((occ, pot, weight, mixes))

    rest = (orbitals, partner, pot, group)
    other_occ = swapped(occ, XH)
    far = project(occ, 0, *rest)
    far = swapped(far, CORE)
    near = project(occ, 1, *rest)
    near, other_occ = lax.optimization_barrier((near, other_occ))
    summed = small_call(join_kernel, jax.ShapeDtypeStruct(near.shape, BF16), near, far)
    intersection = jnp.sum(exchanged(summed, CHIP).astype(F32), axis=0)
    guess = (intersection * weight).astype(BF16)

    given, kept = guess[: nv // nx], guess[nv // nx :]
    guesses = jnp.stack([kept, swapped(given, XH)])
    near_guess = exchanged(jnp.broadcast_to(guesses, (chips, *guesses.shape)), CHIP)
    far_guess = swapped(near_guess, CORE)
    response = respond((occ, other_occ), orbitals, partner, far_guess, near_guess, group, nz)

    out = jax.ShapeDtypeStruct((chips, per_owner, lines, SIDE), BF16)
    columns = small_call(columns_kernel, out, exchanged(response, Z), coul_cols)
    near_cols = exchanged(columns, CHIP)
    far_cols = swapped(near_cols, CORE)
    out = jax.ShapeDtypeStruct((per_owner, lines, SIDE), F32)
    return small_call(rows_kernel, out, near_cols, far_cols, *mixes)


def solution(mesh):
    torus = Mesh(mesh.devices.reshape(8, 2, 4, 2, 2), (Z, XH, Y, XL, CORE))
    return jax.shard_map(
        body,
        mesh=torus,
        in_specs=(P(None, CELL), P(ORB, CELL), P(), P(), P(), P()),
        out_specs=P(ORB, CELL, None),
        check_vma=False,
    )
```

```python
import functools

import jax
import jax.numpy as jnp
from jax import lax
from jax.experimental import pallas as pl
from jax.experimental.pallas import tpu as pltpu
from jax.sharding import Mesh
from jax.sharding import PartitionSpec as P

SIDE = 256
Z, XH, Y, XL, CORE = "z", "x_hi", "y", "x_lo", "core"
CELL = (Y, XL, CORE)
ORB = (Z, XH)
CHIP = (Y, XL)
F32, BF16 = jnp.float32, jnp.bfloat16
HIGH = lax.Precision.HIGHEST
SWAP = ((0, 1), (1, 0))
WHOLE = pl.BlockSpec(memory_space=pltpu.VMEM)
ROOM = pltpu.CompilerParams(vmem_limit_bytes=20 * 2**20)


def swapped(shard, axis):
    return lax.ppermute(shard, axis, SWAP)


def exchanged(parts, axes):
    return lax.all_to_all(parts, axes, split_axis=0, concat_axis=0, tiled=True)


def split_kernel(rows_ref, out_ref):
    width = out_ref.shape[2]
    for k in range(out_ref.shape[0]):
        out_ref[k] = rows_ref[:, k * width : (k + 1) * width]


def pick_kernel(wanted_ref, rows_ref, out_ref):
    count, stored = wanted_ref.shape[0], rows_ref.shape[0]
    label = lax.broadcasted_iota(jnp.int32, (count, stored), 1)
    chosen = jnp.where(wanted_ref[...] == label, 1.0, 0.0).astype(BF16)
    picked = jnp.dot(chosen, rows_ref[...], preferred_element_type=F32).astype(BF16)
    slots = out_ref.shape[1]
    for k in range(out_ref.shape[0]):
        n = k % (count // slots)
        out_ref[k] = picked[n * slots : (n + 1) * slots]


def order_kernel(source_ref, rows_ref, out_ref):
    count = source_ref.shape[0]
    label = lax.broadcasted_iota(jnp.int32, (count, count), 1)
    order = jnp.where(source_ref[...] == label, 1.0, 0.0).astype(BF16)
    out_ref[...] = jnp.dot(order, rows_ref[...], preferred_element_type=F32).astype(BF16)


def join_kernel(near_ref, far_ref, out_ref):
    out_ref[...] = (near_ref[...] + far_ref[...]).astype(out_ref.dtype)


def products(occ, places, parts):
    return jnp.concatenate([occ[n : n + 1, :] * part for n in places for part in parts], axis=0)


def stack_kernel(first_ref, second_ref, *out_refs):
    rows = first_ref.shape[0]
    for ref in out_refs:
        ref[:rows] = first_ref[...]
        ref[rows:] = second_ref[...]


def halves(basis_ref, cut):
    rows = basis_ref.shape[0] // 2
    return basis_ref[:rows, cut], basis_ref[rows:, cut]


def project_kernel(occ_ref, basis_ref, pot_ref, out_ref, *, start, group):
    blocks, _, width = occ_ref.shape
    count, _, lanes = out_ref.shape
    per_step = 16
    outs = per_step // group

    def step(t, carry):
        places = pl.ds(pl.multiple_of(start + t * per_step, per_step), per_step)
        total = None
        for k in range(blocks):
            cut = slice(k * width, (k + 1) * width)
            parts = halves(basis_ref, cut)
            pairs = products(occ_ref[k, places, :], range(per_step), parts)
            term = lax.dot_general(
                pairs, pot_ref[:, cut], (((1,), (1,)), ((), ())), preferred_element_type=F32
            )
            total = term if total is None else total + term
        for n in range(outs):
            out_ref[t * outs + n] = total[n * lanes : (n + 1) * lanes].T
        return carry

    lax.fori_loop(0, count // outs, step, 0)


def project(occ, part, basis, pot, group):
    _, slots, _ = occ.shape
    rows, points = basis.shape
    nv = pot.shape[0]
    half = slots // 2
    return pl.pallas_call(
        functools.partial(project_kernel, start=part * half, group=group),
        in_specs=[WHOLE] * 3,
        out_specs=WHOLE,
        out_shape=jax.ShapeDtypeStruct((half // group, nv, group * rows), F32),
        cost_estimate=pl.CostEstimate(
            flops=2 * half * rows * points * nv, bytes_accessed=4_000_000, transcendentals=0
        ),
        compiler_params=ROOM,
        name="project",
    )(occ, basis, pot)


def respond_kernel(*refs, group):
    *occ_refs, basis_ref, far_ref, near_ref, out_ref = refs
    blocks, _, nv, _ = far_ref.shape
    owners, size, side = out_ref.shape
    per_owner = nv // owners
    per_step = 8

    def step(t, carry):
        lines = []
        for r in range(per_step):
            k = t * per_step + r
            cut = pl.ds(pl.multiple_of(k * side, side), side)
            parts = halves(basis_ref, cut)
            total = None
            for p, occ_ref in enumerate(occ_refs):
                occ = occ_ref[k]
                for h, ref in enumerate((far_ref, near_ref)):
                    for b in range(blocks):
                        base = (h * blocks + b) * group
                        places = range(base, base + group)
                        pairs = products(occ, places, parts[:: 1 - 2 * p])
                        term = jnp.dot(ref[b, p], pairs, preferred_element_type=F32)
                        total = term if total is None else total + term
            lines.append(total)
        rows = per_step * per_owner
        for n in range(owners):
            piece = [line[n * per_owner : (n + 1) * per_owner] for line in lines]
            piece = jnp.concatenate(piece, axis=0).astype(out_ref.dtype)
            out_ref[n, pl.ds(pl.multiple_of(t * rows, rows), rows), :] = piece
        return carry

    lax.fori_loop(0, size // per_owner // per_step, step, 0)


def respond(occs, basis, far, near, group, owners):
    lines, slots, _ = occs[0].shape
    rows, points = basis.shape
    nv = far.shape[2]
    return pl.pallas_call(
        functools.partial(respond_kernel, group=group),
        in_specs=[WHOLE] * (len(occs) + 3),
        out_specs=WHOLE,
        out_shape=jax.ShapeDtypeStruct((owners, lines * nv // owners, SIDE), BF16),
        cost_estimate=pl.CostEstimate(
            flops=2 * len(occs) * slots * rows * points * nv,
            bytes_accessed=6_000_000,
            transcendentals=0,
        ),
        compiler_params=ROOM,
        name="respond",
    )(*occs, basis, far, near)


def columns_kernel(parts_ref, cols_ref, out_ref):
    copies, count, lines, side = out_ref.shape
    size = count * lines
    plane = parts_ref[0].astype(F32)
    for s in range(1, parts_ref.shape[0]):
        plane = plane + parts_ref[s].astype(F32)
    mixed = lax.dot_general(
        plane, cols_ref[...], (((1,), (1,)), ((), ())), precision=HIGH, preferred_element_type=F32
    ).astype(BF16)
    row = lax.broadcasted_iota(jnp.int32, (size, size), 0)
    column = lax.broadcasted_iota(jnp.int32, (size, size), 1)
    source = row % lines * count + row // lines
    swap = jnp.where(source == column, 1.0, 0.0).astype(BF16)
    block = jnp.dot(swap, mixed, preferred_element_type=F32).astype(BF16)
    block = block.reshape(count, lines, side)
    for n in range(copies):
        out_ref[n] = block


def in_three(block):
    high = block.astype(BF16)
    rest = block - high.astype(F32)
    mid = rest.astype(BF16)
    low = (rest - mid.astype(F32)).astype(BF16)
    return high, mid, low


def rows_kernel(near_ref, far_ref, mix_near_ref, mix_far_ref, out_ref):
    chips, count, lines, _ = near_ref.shape
    mixes = [jnp.concatenate(in_three(m[...]), axis=0) for m in (mix_near_ref, mix_far_ref)]
    for n in range(count):
        total = None
        for ref, mix in zip((near_ref, far_ref), mixes):
            block = jnp.concatenate([ref[k, n] for k in range(chips)], axis=0)
            term = jnp.dot(mix, block, preferred_element_type=F32)
            total = term if total is None else total + term
        out_ref[n] = total[:lines] + (total[lines : 2 * lines] + total[2 * lines :])


def small_call(kernel, out, *args):
    return pl.pallas_call(kernel, out_shape=out, compiler_params=ROOM)(*args)


def body(potentials, orbitals, levels, occ_index, coul_rows, coul_cols):
    nv, points = potentials.shape
    mine = orbitals.shape[0]
    norb, nocc = levels.shape[0], occ_index.shape[0]
    nz, nx, ny, nl, nc = (lax.axis_size(a) for a in (Z, XH, Y, XL, CORE))
    z, xh, y, xl, core = (lax.axis_index(a) for a in (Z, XH, Y, XL, CORE))
    chips = ny * nl
    chip = y * nl + xl
    width = points // (nz * nx)
    slots = nocc // nx
    half = slots // nc
    group = half // chips
    lines = points // SIDE
    volume = points * chips * nc
    per_owner = nv // (nz * nx)

    blocks = jax.ShapeDtypeStruct((nz * nx, mine, width), BF16)
    partner = swapped(orbitals, XH)
    by_points = exchanged(small_call(split_kernel, blocks, orbitals), ORB)

    def part_of(values, start, count):
        return lax.dynamic_slice_in_dim(values, start, count)

    starts = [s * slots + c * half for s in range(nx) for c in (1 - core, core)]
    wanted = jnp.concatenate([part_of(occ_index, s, half) for s in starts])[:, None]
    copies = jax.ShapeDtypeStruct((nz * nx, slots, width), BF16)
    spread = small_call(pick_kernel, copies, wanted, by_points.reshape(norb, width))
    occ = exchanged(spread, ORB)

    place = jnp.arange(nv, dtype=jnp.int32)
    side = (xh + 1 + place // (nz * per_owner)) % nx
    source = (place // per_owner % nz * nx + side) * per_owner + place % per_owner
    out = jax.ShapeDtypeStruct(potentials.shape, BF16)
    pot = small_call(order_kernel, out, source[:, None], potentials)

    labels = jnp.arange(norb, dtype=jnp.int32)
    empty = 1.0 - jnp.any(occ_index[:, None] == labels[None, :], axis=0).astype(F32)
    own_slots = part_of(occ_index, xh * slots + core * half + chip * group, group)
    own_levels = jnp.sum(
        jnp.where(own_slots[:, None] == labels[None, :], levels[None, :], 0.0), axis=1
    )
    stored = [(z * nx + n) * mine for n in (xh, 1 - xh)]
    basis_empty = jnp.concatenate([part_of(empty, n, mine) for n in stored])
    basis_levels = jnp.concatenate([part_of(levels, n, mine) for n in stored])
    weight = -2.0 * basis_empty[None, :] / (own_levels[:, None] + basis_levels[None, :])
    weight = (weight / volume).reshape(1, group * nx * mine)

    my_rows = part_of(coul_rows, (chip * nc + core) * lines, lines)
    my_rows = my_rows.reshape(lines, chips, nc, lines)
    mixes = [
        lax.dynamic_index_in_dim(my_rows, c, 2, keepdims=False).reshape(lines, chips * lines)
        for c in (core, 1 - core)
    ]
    out = jax.ShapeDtypeStruct((nx * mine, points), BF16)
    bases = small_call(stack_kernel, [out] * 3, orbitals, partner)
    early = (occ, bases, pot, weight, mixes)
    occ, bases, pot, weight, mixes = lax.optimization_barrier(early)

    other_occ = swapped(occ, XH)
    far = project(occ, 0, bases[0], pot, group)
    far = swapped(far, CORE)
    near = project(occ, 1, bases[1], pot, group)
    near, other_occ = lax.optimization_barrier((near, other_occ))
    summed = small_call(join_kernel, jax.ShapeDtypeStruct(near.shape, BF16), near, far)
    intersection = jnp.sum(exchanged(summed, CHIP).astype(F32), axis=0)
    guess = (intersection * weight).astype(BF16)

    given, kept = guess[: nv // nx], guess[nv // nx :]
    guesses = jnp.stack([kept, swapped(given, XH)])
    near_guess = exchanged(jnp.broadcast_to(guesses, (chips, *guesses.shape)), CHIP)
    far_guess = swapped(near_guess, CORE)
    response = respond((occ, other_occ), bases[2], far_guess, near_guess, group, nz)

    out = jax.ShapeDtypeStruct((chips, per_owner, lines, SIDE), BF16)
    columns = small_call(columns_kernel, out, exchanged(response, Z), coul_cols)
    near_cols = exchanged(columns, CHIP)
    far_cols = swapped(near_cols, CORE)
    out = jax.ShapeDtypeStruct((per_owner, lines, SIDE), F32)
    return small_call(rows_kernel, out, near_cols, far_cols, *mixes)


def solution(mesh):
    torus = Mesh(mesh.devices.reshape(8, 2, 4, 2, 2), (Z, XH, Y, XL, CORE))
    return jax.shard_map(
        body,
        mesh=torus,
        in_specs=(P(None, CELL), P(ORB, CELL), P(), P(), P(), P()),
        out_specs=P(ORB, CELL, None),
        check_vma=False,
    )
```

```python
import functools

import jax
import jax.numpy as jnp
from jax import lax
from jax.experimental import pallas as pl
from jax.experimental.pallas import tpu as pltpu
from jax.sharding import Mesh
from jax.sharding import PartitionSpec as P

SIDE = 256
Z, XH, Y, XL, CORE = "z", "x_hi", "y", "x_lo", "core"
CELL = (Y, XL, CORE)
ORB = (Z, XH)
CHIP = (Y, XL)
F32, BF16 = jnp.float32, jnp.bfloat16
HIGH = lax.Precision.HIGHEST
SWAP = ((0, 1), (1, 0))
WHOLE = pl.BlockSpec(memory_space=pltpu.VMEM)
ROOM = pltpu.CompilerParams(vmem_limit_bytes=20 * 2**20)


def swapped(shard, axis):
    return lax.ppermute(shard, axis, SWAP)


def exchanged(parts, axes):
    return lax.all_to_all(parts, axes, split_axis=0, concat_axis=0, tiled=True)


def split_kernel(rows_ref, out_ref, sems):
    width = out_ref.shape[2]
    copies = [
        pltpu.make_async_copy(rows_ref.at[:, pl.ds(k * width, width)], out_ref.at[k], sems.at[k])
        for k in range(out_ref.shape[0])
    ]
    for copy in copies:
        copy.start()
    for copy in copies:
        copy.wait()


def split(rows, count):
    dims = (count, rows.shape[0], rows.shape[1] // count)
    return pl.pallas_call(
        split_kernel,
        in_specs=[pl.BlockSpec(memory_space=pl.ANY)],
        out_specs=WHOLE,
        out_shape=jax.ShapeDtypeStruct(dims, rows.dtype),
        scratch_shapes=[pltpu.SemaphoreType.DMA((count,))],
        compiler_params=pltpu.CompilerParams(vmem_limit_bytes=60 * 2**20),
        name="split",
    )(rows)


def pick_kernel(wanted_ref, rows_ref, out_ref):
    count, stored = wanted_ref.shape[0], rows_ref.shape[0]
    label = lax.broadcasted_iota(jnp.int32, (count, stored), 1)
    chosen = jnp.where(wanted_ref[...] == label, 1.0, 0.0).astype(BF16)
    picked = jnp.dot(chosen, rows_ref[...], preferred_element_type=F32).astype(BF16)
    slots = out_ref.shape[1]
    for k in range(out_ref.shape[0]):
        n = k % (count // slots)
        out_ref[k] = picked[n * slots : (n + 1) * slots]


def order_kernel(source_ref, rows_ref, out_ref):
    count = source_ref.shape[0]
    label = lax.broadcasted_iota(jnp.int32, (count, count), 1)
    order = jnp.where(source_ref[...] == label, 1.0, 0.0).astype(BF16)
    out_ref[...] = jnp.dot(order, rows_ref[...], preferred_element_type=F32).astype(BF16)


def join_kernel(near_ref, far_ref, out_ref):
    out_ref[...] = (near_ref[...] + far_ref[...]).astype(out_ref.dtype)


def products(occ, places, parts):
    return jnp.concatenate([occ[n : n + 1, :] * part for n in places for part in parts], axis=0)


def stack_kernel(first_ref, second_ref, *out_refs):
    rows = first_ref.shape[0]
    for ref in out_refs:
        ref[:rows] = first_ref[...]
        ref[rows:] = second_ref[...]


def halves(basis_ref, cut):
    rows = basis_ref.shape[0] // 2
    return basis_ref[:rows, cut], basis_ref[rows:, cut]


def project_kernel(occ_ref, basis_ref, pot_ref, out_ref, *occ_copies, start, group):
    for ref in occ_copies:
        ref[...] = occ_ref[...]
    blocks, _, width = occ_ref.shape
    count, _, lanes = out_ref.shape
    per_step = 16
    outs = per_step // group

    def step(t, carry):
        places = pl.ds(pl.multiple_of(start + t * per_step, per_step), per_step)
        total = None
        for k in range(blocks):
            cut = slice(k * width, (k + 1) * width)
            parts = halves(basis_ref, cut)
            pairs = products(occ_ref[k, places, :], range(per_step), parts)
            term = lax.dot_general(
                pairs, pot_ref[:, cut], (((1,), (1,)), ((), ())), preferred_element_type=F32
            )
            total = term if total is None else total + term
        for n in range(outs):
            out_ref[t * outs + n] = total[n * lanes : (n + 1) * lanes].T
        return carry

    lax.fori_loop(0, count // outs, step, 0)


def project(occ, part, basis, pot, group):
    _, slots, _ = occ.shape
    rows, points = basis.shape
    nv = pot.shape[0]
    half = slots // 2
    outs = [jax.ShapeDtypeStruct((half // group, nv, group * rows), F32)]
    outs += [jax.ShapeDtypeStruct(occ.shape, occ.dtype)] * (2 * (1 - part))
    return pl.pallas_call(
        functools.partial(project_kernel, start=part * half, group=group),
        in_specs=[WHOLE] * 3,
        out_specs=[WHOLE] * len(outs),
        out_shape=outs,
        cost_estimate=pl.CostEstimate(
            flops=2 * half * rows * points * nv, bytes_accessed=4_000_000, transcendentals=0
        ),
        compiler_params=ROOM,
        name="project",
    )(occ, basis, pot)


def respond_kernel(*refs, group):
    *occ_refs, basis_ref, far_ref, near_ref, out_ref = refs
    blocks, _, nv, _ = far_ref.shape
    owners, size, side = out_ref.shape
    per_owner = nv // owners
    per_step = 8

    def step(t, carry):
        lines = []
        for r in range(per_step):
            k = t * per_step + r
            cut = pl.ds(pl.multiple_of(k * side, side), side)
            parts = halves(basis_ref, cut)
            total = None
            for p, occ_ref in enumerate(occ_refs):
                occ = occ_ref[k]
                for h, ref in enumerate((far_ref, near_ref)):
                    for b in range(blocks):
                        base = (h * blocks + b) * group
                        places = range(base, base + group)
                        pairs = products(occ, places, parts[:: 1 - 2 * p])
                        term = jnp.dot(ref[b, p], pairs, preferred_element_type=F32)
                        total = term if total is None else total + term
            lines.append(total)
        rows = per_step * per_owner
        for n in range(owners):
            piece = [line[n * per_owner : (n + 1) * per_owner] for line in lines]
            piece = jnp.concatenate(piece, axis=0).astype(out_ref.dtype)
            out_ref[n, pl.ds(pl.multiple_of(t * rows, rows), rows), :] = piece
        return carry

    lax.fori_loop(0, size // per_owner // per_step, step, 0)


def respond(occs, basis, far, near, group, owners):
    lines, slots, _ = occs[0].shape
    rows, points = basis.shape
    nv = far.shape[2]
    return pl.pallas_call(
        functools.partial(respond_kernel, group=group),
        in_specs=[WHOLE] * (len(occs) + 3),
        out_specs=WHOLE,
        out_shape=jax.ShapeDtypeStruct((owners, lines * nv // owners, SIDE), BF16),
        cost_estimate=pl.CostEstimate(
            flops=2 * len(occs) * slots * rows * points * nv,
            bytes_accessed=6_000_000,
            transcendentals=0,
        ),
        compiler_params=ROOM,
        name="respond",
    )(*occs, basis, far, near)


def columns_kernel(parts_ref, cols_ref, out_ref):
    copies, count, lines, side = out_ref.shape
    size = count * lines
    plane = parts_ref[0].astype(F32)
    for s in range(1, parts_ref.shape[0]):
        plane = plane + parts_ref[s].astype(F32)
    mixed = lax.dot_general(
        plane, cols_ref[...], (((1,), (1,)), ((), ())), precision=HIGH, preferred_element_type=F32
    ).astype(BF16)
    row = lax.broadcasted_iota(jnp.int32, (size, size), 0)
    column = lax.broadcasted_iota(jnp.int32, (size, size), 1)
    source = row % lines * count + row // lines
    swap = jnp.where(source == column, 1.0, 0.0).astype(BF16)
    block = jnp.dot(swap, mixed, preferred_element_type=F32).astype(BF16)
    block = block.reshape(count, lines, side)
    for n in range(copies):
        out_ref[n] = block


def in_three(block):
    high = block.astype(BF16)
    rest = block - high.astype(F32)
    mid = rest.astype(BF16)
    low = (rest - mid.astype(F32)).astype(BF16)
    return high, mid, low


def rows_kernel(near_ref, far_ref, mix_near_ref, mix_far_ref, out_ref):
    chips, count, lines, _ = near_ref.shape
    mixes = [jnp.concatenate(in_three(m[...]), axis=0) for m in (mix_near_ref, mix_far_ref)]
    for n in range(count):
        total = None
        for ref, mix in zip((near_ref, far_ref), mixes):
            block = jnp.concatenate([ref[k, n] for k in range(chips)], axis=0)
            term = jnp.dot(mix, block, preferred_element_type=F32)
            total = term if total is None else total + term
        out_ref[n] = total[:lines] + (total[lines : 2 * lines] + total[2 * lines :])


def small_call(kernel, out, *args):
    return pl.pallas_call(kernel, out_shape=out, compiler_params=ROOM)(*args)


def body(potentials, orbitals, levels, occ_index, coul_rows, coul_cols):
    nv, points = potentials.shape
    mine = orbitals.shape[0]
    norb, nocc = levels.shape[0], occ_index.shape[0]
    nz, nx, ny, nl, nc = (lax.axis_size(a) for a in (Z, XH, Y, XL, CORE))
    z, xh, y, xl, core = (lax.axis_index(a) for a in (Z, XH, Y, XL, CORE))
    chips = ny * nl
    chip = y * nl + xl
    width = points // (nz * nx)
    slots = nocc // nx
    half = slots // nc
    group = half // chips
    lines = points // SIDE
    volume = points * chips * nc
    per_owner = nv // (nz * nx)

    partner = swapped(orbitals, XH)
    by_points = exchanged(split(orbitals, nz * nx), ORB)

    def part_of(values, start, count):
        return lax.dynamic_slice_in_dim(values, start, count)

    starts = [s * slots + c * half for s in range(nx) for c in (1 - core, core)]
    wanted = jnp.concatenate([part_of(occ_index, s, half) for s in starts])[:, None]
    copies = jax.ShapeDtypeStruct((nz * nx, slots, width), BF16)
    spread = small_call(pick_kernel, copies, wanted, by_points.reshape(norb, width))
    occ = exchanged(spread, ORB)

    place = jnp.arange(nv, dtype=jnp.int32)
    side = (xh + 1 + place // (nz * per_owner)) % nx
    source = (place // per_owner % nz * nx + side) * per_owner + place % per_owner
    out = jax.ShapeDtypeStruct(potentials.shape, BF16)
    pot = small_call(order_kernel, out, source[:, None], potentials)

    labels = jnp.arange(norb, dtype=jnp.int32)
    empty = 1.0 - jnp.any(occ_index[:, None] == labels[None, :], axis=0).astype(F32)
    own_slots = part_of(occ_index, xh * slots + core * half + chip * group, group)
    own_levels = jnp.sum(
        jnp.where(own_slots[:, None] == labels[None, :], levels[None, :], 0.0), axis=1
    )
    stored = [(z * nx + n) * mine for n in (xh, 1 - xh)]
    basis_empty = jnp.concatenate([part_of(empty, n, mine) for n in stored])
    basis_levels = jnp.concatenate([part_of(levels, n, mine) for n in stored])
    weight = -2.0 * basis_empty[None, :] / (own_levels[:, None] + basis_levels[None, :])
    weight = (weight / volume).reshape(1, group * nx * mine)

    my_rows = part_of(coul_rows, (chip * nc + core) * lines, lines)
    my_rows = my_rows.reshape(lines, chips, nc, lines)
    mixes = [
        lax.dynamic_index_in_dim(my_rows, c, 2, keepdims=False).reshape(lines, chips * lines)
        for c in (core, 1 - core)
    ]
    out = jax.ShapeDtypeStruct((nx * mine, points), BF16)
    bases = small_call(stack_kernel, [out] * 3, orbitals, partner)
    early = (occ, bases, pot, weight, mixes)
    occ, bases, pot, weight, mixes = lax.optimization_barrier(early)

    other_occ = swapped(occ, XH)
    far, *occs = project(occ, 0, bases[0], pot, group)
    far = swapped(far, CORE)
    (near,) = project(occs[0], 1, bases[1], pot, group)
    near, other_occ = lax.optimization_barrier((near, other_occ))
    summed = small_call(join_kernel, jax.ShapeDtypeStruct(near.shape, BF16), near, far)
    intersection = jnp.sum(exchanged(summed, CHIP).astype(F32), axis=0)
    guess = (intersection * weight).astype(BF16)

    given, kept = guess[: nv // nx], guess[nv // nx :]
    guesses = jnp.stack([kept, swapped(given, XH)])
    near_guess = exchanged(jnp.broadcast_to(guesses, (chips, *guesses.shape)), CHIP)
    far_guess = swapped(near_guess, CORE)
    response = respond((occs[1], other_occ), bases[2], far_guess, near_guess, group, nz)

    out = jax.ShapeDtypeStruct((chips, per_owner, lines, SIDE), BF16)
    columns = small_call(columns_kernel, out, exchanged(response, Z), coul_cols)
    near_cols = exchanged(columns, CHIP)
    far_cols = swapped(near_cols, CORE)
    out = jax.ShapeDtypeStruct((per_owner, lines, SIDE), F32)
    return small_call(rows_kernel, out, near_cols, far_cols, *mixes)


def solution(mesh):
    torus = Mesh(mesh.devices.reshape(8, 2, 4, 2, 2), (Z, XH, Y, XL, CORE))
    return jax.shard_map(
        body,
        mesh=torus,
        in_specs=(P(None, CELL), P(ORB, CELL), P(), P(), P(), P()),
        out_specs=P(ORB, CELL, None),
        check_vma=False,
    )
```

```python
import functools

import jax
import jax.numpy as jnp
from jax import lax
from jax.experimental import pallas as pl
from jax.experimental.pallas import tpu as pltpu
from jax.sharding import Mesh
from jax.sharding import PartitionSpec as P

SIDE = 256
Z, XH, Y, XL, CORE = "z", "x_hi", "y", "x_lo", "core"
CELL = (Y, XL, CORE)
ORB = (Z, XH)
CHIP = (Y, XL)
F32, BF16 = jnp.float32, jnp.bfloat16
HIGH = lax.Precision.HIGHEST
SWAP = ((0, 1), (1, 0))
WHOLE = pl.BlockSpec(memory_space=pltpu.VMEM)
ROOM = pltpu.CompilerParams(vmem_limit_bytes=20 * 2**20)


def swapped(shard, axis):
    return lax.ppermute(shard, axis, SWAP)


def exchanged(parts, axes):
    return lax.all_to_all(parts, axes, split_axis=0, concat_axis=0, tiled=True)


def split_kernel(rows_ref, out_ref, sems):
    width = out_ref.shape[2]
    copies = [
        pltpu.make_async_copy(rows_ref.at[:, pl.ds(k * width, width)], out_ref.at[k], sems.at[k])
        for k in range(out_ref.shape[0])
    ]
    for copy in copies:
        copy.start()
    for copy in copies:
        copy.wait()


def split(rows, count):
    dims = (count, rows.shape[0], rows.shape[1] // count)
    return pl.pallas_call(
        split_kernel,
        in_specs=[pl.BlockSpec(memory_space=pl.ANY)],
        out_specs=WHOLE,
        out_shape=jax.ShapeDtypeStruct(dims, rows.dtype),
        scratch_shapes=[pltpu.SemaphoreType.DMA((count,))],
        compiler_params=pltpu.CompilerParams(vmem_limit_bytes=60 * 2**20),
        name="split",
    )(rows)


def pick_kernel(wanted_ref, rows_ref, out_ref):
    count, stored = wanted_ref.shape[0], rows_ref.shape[0]
    label = lax.broadcasted_iota(jnp.int32, (count, stored), 1)
    chosen = jnp.where(wanted_ref[...] == label, 1.0, 0.0).astype(BF16)
    picked = jnp.dot(chosen, rows_ref[...], preferred_element_type=F32).astype(BF16)
    slots = out_ref.shape[1]
    for k in range(out_ref.shape[0]):
        n = k % (count // slots)
        out_ref[k] = picked[n * slots : (n + 1) * slots]


def order_kernel(source_ref, rows_ref, out_ref):
    count = source_ref.shape[0]
    label = lax.broadcasted_iota(jnp.int32, (count, count), 1)
    order = jnp.where(source_ref[...] == label, 1.0, 0.0).astype(BF16)
    out_ref[...] = jnp.dot(order, rows_ref[...], preferred_element_type=F32).astype(BF16)


def join_kernel(near_ref, far_ref, out_ref):
    out_ref[...] = (near_ref[...] + far_ref[...]).astype(out_ref.dtype)


def products(occ, places, parts):
    return jnp.concatenate([occ[n : n + 1, :] * part for n in places for part in parts], axis=0)


def stack_kernel(first_ref, second_ref, *out_refs):
    rows = first_ref.shape[0]
    for ref in out_refs:
        ref[:rows] = first_ref[...]
        ref[rows:] = second_ref[...]


def halves(basis_ref, cut):
    rows = basis_ref.shape[0] // 2
    return basis_ref[:rows, cut], basis_ref[rows:, cut]


def project_kernel(occ_ref, basis_ref, pot_ref, out_ref, *occ_copies, start, group):
    for ref in occ_copies:
        ref[...] = occ_ref[...]
    blocks, _, width = occ_ref.shape
    count, _, lanes = out_ref.shape
    per_step = 16
    outs = per_step // group

    def step(t, carry):
        places = pl.ds(pl.multiple_of(start + t * per_step, per_step), per_step)
        total = None
        for k in range(blocks):
            cut = slice(k * width, (k + 1) * width)
            parts = halves(basis_ref, cut)
            pairs = products(occ_ref[k, places, :], range(per_step), parts)
            term = lax.dot_general(
                pairs, pot_ref[:, cut], (((1,), (1,)), ((), ())), preferred_element_type=F32
            )
            total = term if total is None else total + term
        for n in range(outs):
            out_ref[t * outs + n] = total[n * lanes : (n + 1) * lanes].T
        return carry

    lax.fori_loop(0, count // outs, step, 0)


def project(occ, part, basis, pot, group):
    _, slots, _ = occ.shape
    rows, points = basis.shape
    nv = pot.shape[0]
    half = slots // 2
    outs = [jax.ShapeDtypeStruct((half // group, nv, group * rows), F32)]
    outs += [jax.ShapeDtypeStruct(occ.shape, occ.dtype)] * (3 * (1 - part))
    return pl.pallas_call(
        functools.partial(project_kernel, start=part * half, group=group),
        in_specs=[WHOLE] * 3,
        out_specs=[WHOLE] * len(outs),
        out_shape=outs,
        cost_estimate=pl.CostEstimate(
            flops=2 * half * rows * points * nv, bytes_accessed=4_000_000, transcendentals=0
        ),
        compiler_params=ROOM,
        name="project",
    )(occ, basis, pot)


def respond_kernel(*refs, first, group):
    own_occ, other_occ, basis_ref, guess_ref, *sums, out_ref = refs
    blocks, _, nv, _ = guess_ref.shape
    lines, _, side = own_occ.shape
    per_step = 8

    def step(t, carry):
        totals = []
        for r in range(per_step):
            k = t * per_step + r
            cut = pl.ds(pl.multiple_of(k * side, side), side)
            parts = halves(basis_ref, cut)
            total = sums[0][k] if sums else None
            for p, occ_ref in enumerate((own_occ, other_occ)):
                occ = occ_ref[k]
                for b in range(blocks):
                    places = range(first + b * group, first + (b + 1) * group)
                    pairs = products(occ, places, parts[:: 1 - 2 * p])
                    term = jnp.dot(guess_ref[b, p], pairs, preferred_element_type=F32)
                    total = term if total is None else total + term
            if not sums:
                out_ref[k] = total
            totals.append(total)
        if sums:
            owners = out_ref.shape[0]
            per_owner = nv // owners
            rows = per_step * per_owner
            for n in range(owners):
                piece = [total[n * per_owner : (n + 1) * per_owner] for total in totals]
                piece = jnp.concatenate(piece, axis=0).astype(out_ref.dtype)
                out_ref[n, pl.ds(pl.multiple_of(t * rows, rows), rows), :] = piece
        return carry

    lax.fori_loop(0, lines // per_step, step, 0)


def respond(occs, basis, guess, first, out, group, *sums):
    _, slots, _ = occs[0].shape
    rows, points = basis.shape
    nv = guess.shape[2]
    return pl.pallas_call(
        functools.partial(respond_kernel, first=first, group=group),
        in_specs=[WHOLE] * (4 + len(sums)),
        out_specs=WHOLE,
        out_shape=out,
        cost_estimate=pl.CostEstimate(
            flops=2 * slots * rows * points * nv, bytes_accessed=4_000_000, transcendentals=0
        ),
        compiler_params=ROOM,
        name="respond",
    )(*occs, basis, guess, *sums)


def columns_kernel(parts_ref, cols_ref, out_ref):
    copies, count, lines, side = out_ref.shape
    size = count * lines
    plane = parts_ref[0].astype(F32)
    for s in range(1, parts_ref.shape[0]):
        plane = plane + parts_ref[s].astype(F32)
    mixed = lax.dot_general(
        plane, cols_ref[...], (((1,), (1,)), ((), ())), precision=HIGH, preferred_element_type=F32
    ).astype(BF16)
    row = lax.broadcasted_iota(jnp.int32, (size, size), 0)
    column = lax.broadcasted_iota(jnp.int32, (size, size), 1)
    source = row % lines * count + row // lines
    swap = jnp.where(source == column, 1.0, 0.0).astype(BF16)
    block = jnp.dot(swap, mixed, preferred_element_type=F32).astype(BF16)
    block = block.reshape(count, lines, side)
    for n in range(copies):
        out_ref[n] = block


def in_three(block):
    high = block.astype(BF16)
    rest = block - high.astype(F32)
    mid = rest.astype(BF16)
    low = (rest - mid.astype(F32)).astype(BF16)
    return high, mid, low


def rows_kernel(near_ref, far_ref, mix_near_ref, mix_far_ref, out_ref):
    chips, count, lines, _ = near_ref.shape
    mixes = [jnp.concatenate(in_three(m[...]), axis=0) for m in (mix_near_ref, mix_far_ref)]
    for n in range(count):
        total = None
        for ref, mix in zip((near_ref, far_ref), mixes):
            block = jnp.concatenate([ref[k, n] for k in range(chips)], axis=0)
            term = jnp.dot(mix, block, preferred_element_type=F32)
            total = term if total is None else total + term
        out_ref[n] = total[:lines] + (total[lines : 2 * lines] + total[2 * lines :])


def small_call(kernel, out, *args):
    return pl.pallas_call(kernel, out_shape=out, compiler_params=ROOM)(*args)


def body(potentials, orbitals, levels, occ_index, coul_rows, coul_cols):
    nv, points = potentials.shape
    mine = orbitals.shape[0]
    norb, nocc = levels.shape[0], occ_index.shape[0]
    nz, nx, ny, nl, nc = (lax.axis_size(a) for a in (Z, XH, Y, XL, CORE))
    z, xh, y, xl, core = (lax.axis_index(a) for a in (Z, XH, Y, XL, CORE))
    chips = ny * nl
    chip = y * nl + xl
    width = points // (nz * nx)
    slots = nocc // nx
    half = slots // nc
    group = half // chips
    lines = points // SIDE
    volume = points * chips * nc
    per_owner = nv // (nz * nx)

    partner = swapped(orbitals, XH)
    by_points = exchanged(split(orbitals, nz * nx), ORB)

    def part_of(values, start, count):
        return lax.dynamic_slice_in_dim(values, start, count)

    starts = [s * slots + c * half for s in range(nx) for c in (1 - core, core)]
    wanted = jnp.concatenate([part_of(occ_index, s, half) for s in starts])[:, None]
    copies = jax.ShapeDtypeStruct((nz * nx, slots, width), BF16)
    spread = small_call(pick_kernel, copies, wanted, by_points.reshape(norb, width))
    occ = exchanged(spread, ORB)

    place = jnp.arange(nv, dtype=jnp.int32)
    side = (xh + 1 + place // (nz * per_owner)) % nx
    source = (place // per_owner % nz * nx + side) * per_owner + place % per_owner
    out = jax.ShapeDtypeStruct(potentials.shape, BF16)
    pot = small_call(order_kernel, out, source[:, None], potentials)

    labels = jnp.arange(norb, dtype=jnp.int32)
    empty = 1.0 - jnp.any(occ_index[:, None] == labels[None, :], axis=0).astype(F32)
    own_slots = part_of(occ_index, xh * slots + core * half + chip * group, group)
    own_levels = jnp.sum(
        jnp.where(own_slots[:, None] == labels[None, :], levels[None, :], 0.0), axis=1
    )
    stored = [(z * nx + n) * mine for n in (xh, 1 - xh)]
    basis_empty = jnp.concatenate([part_of(empty, n, mine) for n in stored])
    basis_levels = jnp.concatenate([part_of(levels, n, mine) for n in stored])
    weight = -2.0 * basis_empty[None, :] / (own_levels[:, None] + basis_levels[None, :])
    weight = (weight / volume).reshape(1, group * nx * mine)

    my_rows = part_of(coul_rows, (chip * nc + core) * lines, lines)
    my_rows = my_rows.reshape(lines, chips, nc, lines)
    mixes = [
        lax.dynamic_index_in_dim(my_rows, c, 2, keepdims=False).reshape(lines, chips * lines)
        for c in (core, 1 - core)
    ]
    out = jax.ShapeDtypeStruct((nx * mine, points), BF16)
    bases = small_call(stack_kernel, [out] * 4, orbitals, partner)
    early = (occ, bases, pot, weight, mixes)
    occ, bases, pot, weight, mixes = lax.optimization_barrier(early)

    other_occ = swapped(occ, XH)
    far, *occs = project(occ, 0, bases[0], pot, group)
    far = swapped(far, CORE)
    (near,) = project(occs[0], 1, bases[1], pot, group)
    near, other_occ = lax.optimization_barrier((near, other_occ))
    summed = small_call(join_kernel, jax.ShapeDtypeStruct(near.shape, BF16), near, far)
    intersection = jnp.sum(exchanged(summed, CHIP).astype(F32), axis=0)
    guess = (intersection * weight).astype(BF16)

    given, kept = guess[: nv // nx], guess[nv // nx :]
    guesses = jnp.stack([kept, swapped(given, XH)])
    near_guess = exchanged(jnp.broadcast_to(guesses, (chips, *guesses.shape)), CHIP)
    far_guess = swapped(near_guess, CORE)
    out = jax.ShapeDtypeStruct((lines, nv // nx, SIDE), F32)
    part = respond((occs[1], other_occ), bases[2], near_guess, half, out, group)
    out = jax.ShapeDtypeStruct((nz, lines * per_owner, SIDE), BF16)
    response = respond((occs[2], other_occ), bases[3], far_guess, 0, out, group, part)

    out = jax.ShapeDtypeStruct((chips, per_owner, lines, SIDE), BF16)
    columns = small_call(columns_kernel, out, exchanged(response, Z), coul_cols)
    near_cols = exchanged(columns, CHIP)
    far_cols = swapped(near_cols, CORE)
    out = jax.ShapeDtypeStruct((per_owner, lines, SIDE), F32)
    return small_call(rows_kernel, out, near_cols, far_cols, *mixes)


def solution(mesh):
    torus = Mesh(mesh.devices.reshape(8, 2, 4, 2, 2), (Z, XH, Y, XL, CORE))
    return jax.shard_map(
        body,
        mesh=torus,
        in_specs=(P(None, CELL), P(ORB, CELL), P(), P(), P(), P()),
        out_specs=P(ORB, CELL, None),
        check_vma=False,
    )
```

```python
import functools

import jax
import jax.numpy as jnp
from jax import lax
from jax.experimental import pallas as pl
from jax.experimental.pallas import tpu as pltpu
from jax.sharding import Mesh
from jax.sharding import PartitionSpec as P

SIDE = 256
Z, XH, Y, XL, CORE = "z", "x_hi", "y", "x_lo", "core"
CELL = (Y, XL, CORE)
ORB = (Z, XH)
CHIP = (XL, Y)
SWEEP = (XH, Z)
F32, BF16 = jnp.float32, jnp.bfloat16
HIGH = lax.Precision.HIGHEST
SWAP = ((0, 1), (1, 0))
WHOLE = pl.BlockSpec(memory_space=pltpu.VMEM)
ROOM = pltpu.CompilerParams(vmem_limit_bytes=20 * 2**20)


def swapped(shard, axis):
    return lax.ppermute(shard, axis, SWAP)


def exchanged(parts, axes):
    return lax.all_to_all(parts, axes, split_axis=0, concat_axis=0, tiled=True)


def split_kernel(rows_ref, out_ref, sems):
    width = out_ref.shape[2]
    copies = [
        pltpu.make_async_copy(rows_ref.at[:, pl.ds(k * width, width)], out_ref.at[k], sems.at[k])
        for k in range(out_ref.shape[0])
    ]
    for copy in copies:
        copy.start()
    for copy in copies:
        copy.wait()


def split(rows, count):
    dims = (count, rows.shape[0], rows.shape[1] // count)
    return pl.pallas_call(
        split_kernel,
        in_specs=[pl.BlockSpec(memory_space=pl.ANY)],
        out_specs=WHOLE,
        out_shape=jax.ShapeDtypeStruct(dims, rows.dtype),
        scratch_shapes=[pltpu.SemaphoreType.DMA((count,))],
        compiler_params=pltpu.CompilerParams(vmem_limit_bytes=60 * 2**20),
        name="split",
    )(rows)


def pick_kernel(wanted_ref, rows_ref, out_ref):
    count, stored = wanted_ref.shape[0], rows_ref.shape[0]
    label = lax.broadcasted_iota(jnp.int32, (count, stored), 1)
    chosen = jnp.where(wanted_ref[...] == label, 1.0, 0.0).astype(BF16)
    picked = jnp.dot(chosen, rows_ref[...], preferred_element_type=F32).astype(BF16)
    slots = out_ref.shape[1]
    for k in range(out_ref.shape[0]):
        n = k * (count // slots) // out_ref.shape[0]
        out_ref[k] = picked[n * slots : (n + 1) * slots]


def order_kernel(source_ref, rows_ref, out_ref):
    count = source_ref.shape[0]
    label = lax.broadcasted_iota(jnp.int32, (count, count), 1)
    order = jnp.where(source_ref[...] == label, 1.0, 0.0).astype(BF16)
    out_ref[...] = jnp.dot(order, rows_ref[...], preferred_element_type=F32).astype(BF16)


def join_kernel(near_ref, far_ref, out_ref):
    out_ref[...] = (near_ref[...] + far_ref[...]).astype(out_ref.dtype)


def products(occ, places, parts):
    return jnp.concatenate([occ[n : n + 1, :] * part for n in places for part in parts], axis=0)


def stack_kernel(first_ref, second_ref, *out_refs):
    rows = first_ref.shape[0]
    for ref in out_refs:
        ref[:rows] = first_ref[...]
        ref[rows:] = second_ref[...]


def halves(basis_ref, cut):
    rows = basis_ref.shape[0] // 2
    return basis_ref[:rows, cut], basis_ref[rows:, cut]


def project_kernel(occ_ref, basis_ref, pot_ref, out_ref, *occ_copies, start, group):
    for ref in occ_copies:
        ref[...] = occ_ref[...]
    blocks, _, width = occ_ref.shape
    count, _, lanes = out_ref.shape
    per_step = 16
    outs = per_step // group

    def step(t, carry):
        places = pl.ds(pl.multiple_of(start + t * per_step, per_step), per_step)
        total = None
        for k in range(blocks):
            cut = slice(k * width, (k + 1) * width)
            parts = halves(basis_ref, cut)
            pairs = products(occ_ref[k, places, :], range(per_step), parts)
            term = lax.dot_general(
                pairs, pot_ref[:, cut], (((1,), (1,)), ((), ())), preferred_element_type=F32
            )
            total = term if total is None else total + term
        for n in range(outs):
            out_ref[t * outs + n] = total[n * lanes : (n + 1) * lanes].T
        return carry

    lax.fori_loop(0, count // outs, step, 0)


def project(occ, part, basis, pot, group):
    _, slots, _ = occ.shape
    rows, points = basis.shape
    nv = pot.shape[0]
    half = slots // 2
    outs = [jax.ShapeDtypeStruct((half // group, nv, group * rows), F32)]
    outs += [jax.ShapeDtypeStruct(occ.shape, occ.dtype)] * (3 * (1 - part))
    return pl.pallas_call(
        functools.partial(project_kernel, start=part * half, group=group),
        in_specs=[WHOLE] * 3,
        out_specs=[WHOLE] * len(outs),
        out_shape=outs,
        cost_estimate=pl.CostEstimate(
            flops=2 * half * rows * points * nv, bytes_accessed=4_000_000, transcendentals=0
        ),
        compiler_params=ROOM,
        name="project",
    )(occ, basis, pot)


def respond_kernel(*refs, first, group):
    own_occ, other_occ, basis_ref, guess_ref, *sums, out_ref = refs
    blocks, _, nv, _ = guess_ref.shape
    lines, _, side = own_occ.shape
    per_step = 16

    def step(t, carry):
        totals = []
        for r in range(per_step):
            k = t * per_step + r
            cut = pl.ds(pl.multiple_of(k * side, side), side)
            parts = halves(basis_ref, cut)
            total = sums[0][k] if sums else None
            for p, occ_ref in enumerate((own_occ, other_occ)):
                occ = occ_ref[k]
                for b in range(blocks):
                    places = range(first + b * group, first + (b + 1) * group)
                    pairs = products(occ, places, parts[:: 1 - 2 * p])
                    term = jnp.dot(guess_ref[b, p], pairs, preferred_element_type=F32)
                    total = term if total is None else total + term
            if not sums:
                out_ref[k] = total
            totals.append(total)
        if sums:
            owners = out_ref.shape[0]
            per_owner = nv // owners
            rows = per_step * per_owner
            for n in range(owners):
                piece = [total[n * per_owner : (n + 1) * per_owner] for total in totals]
                piece = jnp.concatenate(piece, axis=0).astype(out_ref.dtype)
                out_ref[n, pl.ds(pl.multiple_of(t * rows, rows), rows), :] = piece
        return carry

    lax.fori_loop(0, lines // per_step, step, 0)


def respond(occs, basis, guess, first, out, group, *sums):
    _, slots, _ = occs[0].shape
    rows, points = basis.shape
    nv = guess.shape[2]
    return pl.pallas_call(
        functools.partial(respond_kernel, first=first, group=group),
        in_specs=[WHOLE] * (4 + len(sums)),
        out_specs=WHOLE,
        out_shape=out,
        cost_estimate=pl.CostEstimate(
            flops=2 * slots * rows * points * nv, bytes_accessed=4_000_000, transcendentals=0
        ),
        compiler_params=ROOM,
        name="respond",
    )(*occs, basis, guess, *sums)


def columns_kernel(parts_ref, cols_ref, out_ref):
    copies, count, lines, side = out_ref.shape
    size = count * lines
    plane = parts_ref[0].astype(F32)
    for s in range(1, parts_ref.shape[0]):
        plane = plane + parts_ref[s].astype(F32)
    mixed = lax.dot_general(
        plane, cols_ref[...], (((1,), (1,)), ((), ())), precision=HIGH, preferred_element_type=F32
    ).astype(BF16)
    row = lax.broadcasted_iota(jnp.int32, (size, size), 0)
    column = lax.broadcasted_iota(jnp.int32, (size, size), 1)
    source = row % lines * count + row // lines
    swap = jnp.where(source == column, 1.0, 0.0).astype(BF16)
    block = jnp.dot(swap, mixed, preferred_element_type=F32).astype(BF16)
    block = block.reshape(count, lines, side)
    for n in range(copies):
        out_ref[n] = block


def in_three(block):
    high = block.astype(BF16)
    rest = block - high.astype(F32)
    mid = rest.astype(BF16)
    low = (rest - mid.astype(F32)).astype(BF16)
    return high, mid, low


def rows_kernel(near_ref, far_ref, mix_near_ref, mix_far_ref, out_ref):
    chips, count, lines, _ = near_ref.shape
    mixes = [jnp.concatenate(in_three(m[...]), axis=0) for m in (mix_near_ref, mix_far_ref)]
    for n in range(count):
        total = None
        for ref, mix in zip((near_ref, far_ref), mixes):
            block = jnp.concatenate([ref[k, n] for k in range(chips)], axis=0)
            term = jnp.dot(mix, block, preferred_element_type=F32)
            total = term if total is None else total + term
        out_ref[n] = total[:lines] + (total[lines : 2 * lines] + total[2 * lines :])


def small_call(kernel, out, *args):
    return pl.pallas_call(kernel, out_shape=out, compiler_params=ROOM)(*args)


def body(potentials, orbitals, levels, occ_index, coul_rows, coul_cols):
    nv, points = potentials.shape
    mine = orbitals.shape[0]
    norb, nocc = levels.shape[0], occ_index.shape[0]
    nz, nx, ny, nl, nc = (lax.axis_size(a) for a in (Z, XH, Y, XL, CORE))
    z, xh, y, xl, core = (lax.axis_index(a) for a in (Z, XH, Y, XL, CORE))
    chips = ny * nl
    chip = xl * ny + y
    width = points // (nz * nx)
    slots = nocc // nx
    half = slots // nc
    group = half // chips
    lines = points // SIDE
    volume = points * chips * nc
    per_owner = nv // (nz * nx)

    partner = swapped(orbitals, XH)
    by_points = exchanged(split(orbitals, nz * nx), SWEEP)

    def part_of(values, start, count):
        return lax.dynamic_slice_in_dim(values, start, count)

    starts = [s * slots + c * half for s in range(nx) for c in (1 - core, core)]
    wanted = jnp.concatenate([part_of(occ_index, s, half) for s in starts])
    group_of = wanted // mine
    wanted = (group_of % nx * nz + group_of // nx) * mine + wanted % mine
    wanted = wanted[:, None]
    copies = jax.ShapeDtypeStruct((nz * nx, slots, width), BF16)
    spread = small_call(pick_kernel, copies, wanted, by_points.reshape(norb, width))
    occ = exchanged(spread, SWEEP)

    place = jnp.arange(nv, dtype=jnp.int32)
    side = (xh + 1 + place // (nz * per_owner)) % nx
    source = (place // per_owner % nz * nx + side) * per_owner + place % per_owner
    out = jax.ShapeDtypeStruct(potentials.shape, BF16)
    pot = small_call(order_kernel, out, source[:, None], potentials)

    labels = jnp.arange(norb, dtype=jnp.int32)
    empty = 1.0 - jnp.any(occ_index[:, None] == labels[None, :], axis=0).astype(F32)
    own_slots = part_of(occ_index, xh * slots + core * half + chip * group, group)
    own_levels = jnp.sum(
        jnp.where(own_slots[:, None] == labels[None, :], levels[None, :], 0.0), axis=1
    )
    stored = [(z * nx + n) * mine for n in (xh, 1 - xh)]
    basis_empty = jnp.concatenate([part_of(empty, n, mine) for n in stored])
    basis_levels = jnp.concatenate([part_of(levels, n, mine) for n in stored])
    weight = -2.0 * basis_empty[None, :] / (own_levels[:, None] + basis_levels[None, :])
    weight = (weight / volume).reshape(1, group * nx * mine)

    my_rows = part_of(coul_rows, ((y * nl + xl) * nc + core) * lines, lines)
    my_rows = jnp.swapaxes(my_rows.reshape(lines, ny, nl, nc, lines), 1, 2)
    my_rows = my_rows.reshape(lines, chips, nc, lines)
    mixes = [
        lax.dynamic_index_in_dim(my_rows, c, 2, keepdims=False).reshape(lines, chips * lines)
        for c in (core, 1 - core)
    ]
    out = jax.ShapeDtypeStruct((nx * mine, points), BF16)
    bases = small_call(stack_kernel, [out] * 4, orbitals, partner)
    early = (occ, bases, pot, weight, mixes)
    occ, bases, pot, weight, mixes = lax.optimization_barrier(early)

    other_occ = swapped(occ, XH)
    far, *occs = project(occ, 0, bases[0], pot, group)
    far = swapped(far, CORE)
    (near,) = project(occs[0], 1, bases[1], pot, group)
    near, other_occ = lax.optimization_barrier((near, other_occ))
    summed = small_call(join_kernel, jax.ShapeDtypeStruct(near.shape, BF16), near, far)
    intersection = jnp.sum(exchanged(summed, CHIP).astype(F32), axis=0)
    guess = (intersection * weight).astype(BF16)

    given, kept = guess[: nv // nx], guess[nv // nx :]
    guesses = jnp.stack([kept, swapped(given, XH)])
    near_guess = exchanged(jnp.broadcast_to(guesses, (chips, *guesses.shape)), CHIP)
    far_guess = swapped(near_guess, CORE)
    out = jax.ShapeDtypeStruct((lines, nv // nx, SIDE), F32)
    part = respond((occs[1], other_occ), bases[2], near_guess, half, out, group)
    out = jax.ShapeDtypeStruct((nz, lines * per_owner, SIDE), BF16)
    response = respond((occs[2], other_occ), bases[3], far_guess, 0, out, group, part)

    out = jax.ShapeDtypeStruct((chips, per_owner, lines, SIDE), BF16)
    columns = small_call(columns_kernel, out, exchanged(response, Z), coul_cols)
    near_cols = exchanged(columns, CHIP)
    far_cols = swapped(near_cols, CORE)
    out = jax.ShapeDtypeStruct((per_owner, lines, SIDE), F32)
    return small_call(rows_kernel, out, near_cols, far_cols, *mixes)


def solution(mesh):
    torus = Mesh(mesh.devices.reshape(8, 2, 4, 2, 2), (Z, XH, Y, XL, CORE))
    return jax.shard_map(
        body,
        mesh=torus,
        in_specs=(P(None, CELL), P(ORB, CELL), P(), P(), P(), P()),
        out_specs=P(ORB, CELL, None),
        check_vma=False,
    )
```
